32 devices in a mesh: gx: 4 (over y, x), gy: 8 (over z, core).
Axes of the slice: x: 2, y: 2, z: 4, core: 2. Of those that a mesh axis runs over, the one named last changes fastest.
Arguments:
- positions: float32 [3, 65536], P(None, ('gx', 'gy')), may hold values from 0 to 4
- node_moments: float32 [10, 16384], P(None, ('gx', 'gy')), as said below
- slot_of: int32 [32, 2048], P(('gx', 'gy')), may hold values from 0 to 2047, each once within a row
- block_list: int32 [512, 16], P(('gx', 'gy')), may hold values from 0 to 127, as said below
- tile_counts: int32 [512], P(('gx', 'gy')), may hold values from 1 to 16, as said below
Outputs:
- accel: float32 [3, 65536], P(None, ('gx', 'gy'))
The draws below stay inside these ranges and needn't reach their ends.
Inputs may be any that keep to these rules, and one draw needn't show every extreme that they name: `block_list`: each row names 16 different node blocks; only a tile's first tile_counts entries are used. `tile_counts`: some tile of every draw uses all 16 slots. `node_moments`: masses lie in 0.02 to 0.2 and centres in 0 to 4.
All inputs are finite; a program needn't handle non-finite values.
Results may differ from the reference program's by a relative error of at most 0.0003.
Values sent between devices are 32-bit elements; how exact they have to be, the bound alone decides.
No kernel may reach another device: no remote copies, remote signals or barrier semaphores. Data moves between devices by JAX's collectives and lax.ppermute only.
A program may use at most 64 MiB of HBM per device.

```python
import math
import jax
import jax.numpy as jnp
from jax import lax

PART_DEV = 2048
TILE = 128
BLOCK = 128
LIST = 16
TILES_DEV = 16
TILES = 512
PARTS_SIZE = 65536
NODES = 16384
DEVICES = 32


def draw_node_moments(key, part):
    mass_key = jax.random.fold_in(key, 11)
    centre_key = jax.random.fold_in(key, 12)
    quad_key = jax.random.fold_in(key, 13)
    mass = jnp.exp(jax.random.uniform(mass_key, (1, NODES), jnp.float32, math.log(0.02), math.log(0.2)))
    centre = jax.random.uniform(centre_key, (3, NODES), jnp.float32, 0.0, 4.0)
    quad = 0.05 * jax.random.normal(quad_key, (6, NODES), jnp.float32)
    return jnp.concatenate([mass, centre, quad], axis=0).astype(jnp.float32)


def draw_block_list(key, part):
    score_key = jax.random.fold_in(key, 21)
    total_blocks = NODES // BLOCK
    scores = jax.random.randint(score_key, (TILES, total_blocks), 0, 2 ** 18, jnp.int32)
    scores = scores * total_blocks + jnp.arange(total_blocks, dtype=jnp.int32)[None, :]
    chosen = jax.lax.top_k(scores, LIST)[1]
    return chosen.astype(jnp.int32)


def draw_tile_counts(key, part):
    level_key = jax.random.fold_in(key, 31)
    count_key = jax.random.fold_in(key, 32)
    level = jax.random.randint(level_key, (DEVICES, 1), max(LIST // 4, 1), LIST + 1, jnp.int32)
    counts = jax.random.randint(count_key, (DEVICES, TILES_DEV), 1, level + 1, jnp.int32)
    counts = counts.at[0, 0].set(LIST)
    return counts.reshape(TILES).astype(jnp.int32)


def steps_of(rng, extent, cuts, low, largest):
    factor_of = 1.0
    for position, shards_of in cuts:
        steps = jax.random.uniform(jax.random.fold_in(jax.random.fold_in(rng, 6), position), (shards_of,), jnp.float32, low / len(cuts), largest / len(cuts))
        factor_of = factor_of * jnp.repeat(jnp.exp(steps), extent[position] // shards_of).reshape((-1,) + (1,) * (len(extent) - 1 - position))
    return factor_of


def setup_inputs(seed: int = 0) -> dict:
    streams_of = jax.random.split(jax.random.key(seed), 6)
    positions = jnp.clip(4.0 * jax.random.uniform(streams_of[0], (3, PARTS_SIZE), jnp.float32) ** steps_of(streams_of[0], (3, PARTS_SIZE), ((1, 32),), -0.2, 0.2), 0.0, 4.0)
    node_moments = draw_node_moments(jax.random.fold_in(streams_of[5], 71), 0)
    slot_of = jax.vmap(lambda own: jax.random.permutation(own, PART_DEV))(jax.random.split(streams_of[2], DEVICES)).reshape((DEVICES, PART_DEV)).astype(jnp.int32)
    block_list = draw_block_list(jax.random.fold_in(streams_of[5], 71), 0)
    tile_counts = draw_tile_counts(jax.random.fold_in(streams_of[5], 71), 0)
    return {"positions": positions, "node_moments": node_moments, "slot_of": slot_of, "block_list": block_list, "tile_counts": tile_counts}


split_a = 0.5
soft_sq = 0.25

def pair_sum(tiled, near):
    delta = tiled[:, :, :, None] - near[1:4, :, None, :]
    mass = near[0][:, None, :]
    qxx = near[4][:, None, :]
    qyy = near[5][:, None, :]
    qzz = near[6][:, None, :]
    qxy = near[7][:, None, :]
    qxz = near[8][:, None, :]
    qyz = near[9][:, None, :]
    dxv = delta[0]
    dyv = delta[1]
    dzv = delta[2]
    dist_sq = dxv * dxv + dyv * dyv + dzv * dzv + soft_sq
    dist = jnp.sqrt(dist_sq)
    expo = jnp.exp(-split_a * split_a * dist_sq)
    root_pi = math.sqrt(math.pi)
    zeroth = jax.scipy.special.erfc(split_a * dist) / dist
    first = (zeroth + 2.0 * split_a / root_pi * expo) / dist_sq
    second = (3.0 * first + 4.0 * split_a ** 3 / root_pi * expo) / dist_sq
    third = (5.0 * second + 8.0 * split_a ** 5 / root_pi * expo) / dist_sq
    quad_x = qxx * dxv + qxy * dyv + qxz * dzv
    quad_y = qxy * dxv + qyy * dyv + qyz * dzv
    quad_z = qxz * dxv + qyz * dyv + qzz * dzv
    inner = dxv * quad_x + dyv * quad_y + dzv * quad_z
    radial = -mass * first - 0.5 * third * inner + 0.5 * second * (qxx + qyy + qzz)
    force_x = lax.optimization_barrier(jnp.sum(radial * dxv + second * quad_x, axis=-1))
    force_y = lax.optimization_barrier(jnp.sum(radial * dyv + second * quad_y, axis=-1))
    force_z = lax.optimization_barrier(jnp.sum(radial * dzv + second * quad_z, axis=-1))
    return jnp.stack([force_x, force_y, force_z])

def tile_forces(tiled, blocks, lists, counts, trips):

    def slot_term(step, total):
        ids = lax.dynamic_index_in_dim(lists, step, 1, keepdims=False)
        near = jnp.take(blocks, ids, axis=1)
        live = (step < counts).astype(jnp.float32)
        return total + pair_sum(tiled, near) * live[None, :, None]
    start = jnp.zeros(tiled.shape, jnp.float32)
    return lax.fori_loop(0, trips, slot_term, start)

def reference(positions, node_moments, slot_of, block_list, tile_counts):
    blocks = node_moments.reshape(10, -1, BLOCK)
    own_pos = jnp.transpose(positions.reshape(3, DEVICES, PART_DEV), (1, 0, 2))
    own_lists = block_list.reshape(DEVICES, TILES_DEV, LIST)
    own_counts = tile_counts.reshape(DEVICES, TILES_DEV)

    def one_device(items):
        pos, slots, lists, counts = items
        tiled = jnp.zeros(pos.shape, jnp.float32).at[:, slots].set(pos).reshape(3, TILES_DEV, TILE)
        forces = tile_forces(tiled, blocks, lists, counts, LIST).reshape(3, PART_DEV)
        return forces[:, slots]
    result = lax.map(one_device, (own_pos, slot_of, own_lists, own_counts))
    return jnp.transpose(result, (1, 0, 2)).reshape(3, DEVICES * PART_DEV)
```

```python
import functools
import math

import jax
import jax.numpy as jnp
from jax import lax
from jax.experimental import pallas as pl
from jax.experimental.pallas import tpu as pltpu
from jax.sharding import PartitionSpec as P

LANES = 128
SUBS = 8
split_a = 0.5
soft_sq = 0.25
root_pi = math.sqrt(math.pi)

ERFC_BIAS = 0.15
ERFC_POLY = (
    0.565651365,
    -0.0323440266,
    1.41906215,
    -1.34343713,
    0.938636763,
    -0.36025162,
    0.0669870813,
)


def thirds(value):
    top = value.astype(jnp.bfloat16)
    rest = value - top.astype(jnp.float32)
    mid = rest.astype(jnp.bfloat16)
    low = (rest - mid.astype(jnp.float32)).astype(jnp.bfloat16)
    return top, mid, low


def hot_lanes(slots, count):
    lane = lax.bitwise_and(slots, LANES - 1)
    rows = lax.broadcasted_iota(jnp.int32, (LANES, count), 0)
    return jnp.where(rows == lane, 1.0, 0.0).astype(jnp.bfloat16)


def prep_kernel(pos_ref, slot_ref, tiled_ref):
    count = pos_ref.shape[1]
    tiles = count // LANES
    slots = slot_ref[...]
    owner = lax.broadcasted_iota(jnp.int32, (tiles, count), 0) == lax.shift_right_logical(slots, 7)
    hot = hot_lanes(slots, count)
    for c in range(3):
        value = pos_ref[c : c + 1, :]
        total = None
        for part in thirds(value):
            rows = jnp.where(owner, part.astype(jnp.float32), 0.0).astype(jnp.bfloat16)
            got = lax.dot_general(
                rows, hot, (((1,), (1,)), ((), ())), preferred_element_type=jnp.float32
            )
            total = got if total is None else total + got
        tiled_ref[c] = total


def pair_rows(x, y, z, node):
    mass, cx, cy, cz, qxx, qyy, qzz, qxy, qxz, qyz, trace = node
    dx = x - cx
    dy = y - cy
    dz = z - cz
    dist_sq = dx * dx + dy * dy + (dz * dz + soft_sq)
    inv = lax.rsqrt(dist_sq)
    inv_sq = inv * inv
    expo = jnp.exp(-split_a * split_a * dist_sq)
    arg = lax.rsqrt(dist_sq + ERFC_BIAS)
    poly = jnp.full_like(arg, ERFC_POLY[-1])
    for coef in ERFC_POLY[-2::-1]:
        poly = poly * arg + coef
    first = poly * inv_sq
    second = (first + (4.0 * split_a**3 / root_pi / 3.0)) * inv_sq
    third = (second + (8.0 * split_a**5 / root_pi / 15.0)) * inv_sq
    quad_x = qxx * dx + qxy * dy + qxz * dz
    quad_y = qxy * dx + qyy * dy + qyz * dz
    quad_z = qxz * dx + qyz * dy + qzz * dz
    inner = 2.5 * (dx * quad_x + dy * quad_y + dz * quad_z)
    radial = second * trace - mass * first - third * inner
    radial = radial * expo
    second = second * expo
    return (
        radial * dx + second * quad_x,
        radial * dy + second * quad_y,
        radial * dz + second * quad_z,
    )


def main_kernel(
    gx, gy, lists_ref, counts_ref, tiled_ref, slot_ref, nodes_ref, out_ref, spread, acc, force
):
    count = slot_ref.shape[1]
    tiles = count // LANES
    each = nodes_ref.shape[1] * 4 // 5 // SUBS

    def one_tile(t, carry):
        for c in range(3):
            row = tiled_ref[c, pl.ds(t, 1), :]
            spread[c] = jnp.broadcast_to(row, (LANES, LANES)).T
            acc[c] = jnp.zeros((LANES, LANES), jnp.float32)

        def one_slot(k, carry):
            block = lists_ref[t, k]
            dev = lax.div(block, each)
            j = lax.rem(block, each)
            place = lax.rem(dev, gy) * gx + lax.div(dev, gy)
            rows = [nodes_ref[place, pl.ds(j * SUBS + i, 1), :] for i in range(8)]
            rows.append(nodes_ref[place, pl.ds(each * SUBS + j, 1), :])
            rows.append(nodes_ref[place, pl.ds(each * SUBS + each + j, 1), :])
            trace = (rows[4] + rows[5] + rows[6]) * 1.5
            rows = rows[:4] + [r * 3.0 for r in rows[4:]]
            node = [jnp.broadcast_to(r, (SUBS, LANES)) for r in rows + [trace]]
            for g in range(LANES // SUBS):
                at = pl.ds(g * SUBS, SUBS)
                fx, fy, fz = pair_rows(
                    spread[0, at, :], spread[1, at, :], spread[2, at, :], node
                )
                acc[0, at, :] += fx
                acc[1, at, :] += fy
                acc[2, at, :] += fz
            return carry

        lax.fori_loop(0, counts_ref[t], one_slot, 0)
        for c in range(3):
            force[pl.ds(c * tiles + t, 1), :] = jnp.sum(acc[c].T, axis=0, keepdims=True)
        return carry

    lax.fori_loop(0, tiles, one_tile, 0)
    slots = slot_ref[...]
    owner = lax.broadcasted_iota(jnp.int32, (tiles, count), 0) == lax.shift_right_logical(slots, 7)
    hot = hot_lanes(slots, count)
    for c in range(3):
        mine = force[c * tiles : (c + 1) * tiles, :]
        total = None
        for part in thirds(mine):
            got = jnp.dot(part, hot, preferred_element_type=jnp.float32)
            total = got if total is None else total + got
        out_ref[c : c + 1, :] = jnp.sum(jnp.where(owner, total, 0.0), axis=0, keepdims=True)


def shards(gx, gy, positions, node_moments, slot_of, block_list, tile_counts):
    count = positions.shape[1]
    tiles = count // LANES
    nodes = node_moments.shape[1]
    each = nodes // LANES
    packed = jnp.concatenate(
        [
            node_moments[:8].reshape(8, each, LANES).transpose(1, 0, 2).reshape(8 * each, LANES),
            node_moments[8:].reshape(2 * each, LANES),
        ],
        axis=0,
    )
    tiled = pl.pallas_call(
        prep_kernel,
        out_shape=jax.ShapeDtypeStruct((3, tiles, LANES), jnp.float32),
        in_specs=[pl.BlockSpec(memory_space=pltpu.VMEM)] * 2,
        out_specs=pl.BlockSpec(memory_space=pltpu.VMEM),
    )(positions, slot_of)
    every = lax.all_gather(packed, "gx", axis=0)
    every = lax.all_gather(every, "gy", axis=0)
    every = every.reshape(gx * gy, 10 * each, LANES)
    return pl.pallas_call(
        functools.partial(main_kernel, gx, gy),
        out_shape=jax.ShapeDtypeStruct((3, count), jnp.float32),
        in_specs=[pl.BlockSpec(memory_space=pltpu.SMEM)] * 2
        + [pl.BlockSpec(memory_space=pltpu.VMEM)] * 3,
        out_specs=pl.BlockSpec(memory_space=pltpu.VMEM),
        scratch_shapes=[
            pltpu.VMEM((3, LANES, LANES), jnp.float32),
            pltpu.VMEM((3, LANES, LANES), jnp.float32),
            pltpu.VMEM((3 * tiles, LANES), jnp.float32),
        ],
    )(block_list, tile_counts, tiled, slot_of, every)


def solution(mesh):
    placed = (
        P(None, ("gx", "gy")),
        P(None, ("gx", "gy")),
        P(("gx", "gy"), None),
        P(("gx", "gy"), None),
        P(("gx", "gy")),
    )
    return jax.shard_map(
        functools.partial(shards, mesh.shape["gx"], mesh.shape["gy"]),
        mesh=mesh,
        in_specs=placed,
        out_specs=P(None, ("gx", "gy")),
        check_vma=False,
    )
```

```python
import functools
import math

import jax
import jax.numpy as jnp
from jax import lax
from jax.experimental import pallas as pl
from jax.experimental.pallas import tpu as pltpu
from jax.sharding import PartitionSpec as P

LANES = 128
SUBS = 8
PAIRS = 2
FEATURES = 48
WEIGHTS = 40
split_a = 0.5
soft_sq = 0.25
root_pi = math.sqrt(math.pi)
B2_CONST = 4.0 * split_a**3 / root_pi / 3.0
B3_CONST = 8.0 * split_a**5 / root_pi / 15.0
EXP2_SCALE = -split_a * split_a / math.log(2.0)

ERFC_BIAS = 0.15
ERFC_POLY = (
    0.565651365,
    -0.0323440266,
    1.41906215,
    -1.34343713,
    0.938636763,
    -0.36025162,
    0.0669870813,
)


def thirds(value):
    top = value.astype(jnp.bfloat16).astype(jnp.float32)
    rest = value - top
    mid = rest.astype(jnp.bfloat16).astype(jnp.float32)
    low = (rest - mid).astype(jnp.bfloat16).astype(jnp.float32)
    return top, mid, low


def quotient(value, by):
    if by & (by - 1) == 0:
        return lax.shift_right_logical(value, by.bit_length() - 1)
    return lax.div(value, by)


def hot_lanes(slots, count):
    lane = lax.bitwise_and(slots, LANES - 1)
    rows = lax.broadcasted_iota(jnp.int32, (LANES, count), 0)
    return jnp.where(rows == lane, 1.0, 0.0).astype(jnp.bfloat16)


def owners(slots, tiles, count):
    rows = lax.broadcasted_iota(jnp.int32, (tiles, count), 0)
    return rows == lax.shift_right_logical(slots, 7)


def prep_kernel(pos_ref, slot_ref, tiled_ref, origin_ref, left_ref, rows_ref):
    count = pos_ref.shape[1]
    tiles = count // LANES
    slots = slot_ref[...]
    owner = owners(slots, tiles, count)
    hot = hot_lanes(slots, count)
    place = []
    for c in range(3):
        value = pos_ref[c : c + 1, :]
        origin = jnp.sum(value, axis=1, keepdims=True) * (1.0 / count)
        origin_ref[c : c + 1, :] = jnp.broadcast_to(origin, (1, LANES))
        value = value - origin
        total = None
        for part in thirds(value):
            rows = jnp.where(owner, part, 0.0).astype(jnp.bfloat16)
            got = lax.dot_general(
                rows, hot, (((1,), (1,)), ((), ())), preferred_element_type=jnp.float32
            )
            total = got if total is None else total + got
        tiled_ref[c] = total
        place.append(total)
    x, y, z = place
    one = jnp.ones_like(x)
    zero = jnp.zeros_like(x)
    terms = [x, y, z, one, x * x + y * y + (z * z + soft_sq), x, y, z]
    terms += [x * x, y * y, z * z, x * y, x * z, y * z, one, zero]
    for i, term in enumerate(terms):
        top, mid, low = thirds(term)
        for s, part in enumerate((top, top, top, mid, mid, low)):
            rows_ref[pl.ds(s * 16 + i, tiles, stride=LANES), :] = part
    for s in range(96, LANES):
        rows_ref[pl.ds(s, tiles, stride=LANES), :] = zero
    for t in range(tiles):
        left_ref[t] = rows_ref[pl.ds(t * LANES, LANES), :].T.astype(jnp.bfloat16)


def node_features(origin_ref, nodes_ref, feats_ref, weights_ref):
    devices, rows, _ = nodes_ref.shape
    each = rows // 10
    group = max(1, SUBS // each)
    wide = group * each
    shape = (wide, LANES)
    centre = [jnp.broadcast_to(origin_ref[c : c + 1, :], shape) for c in range(3)]

    def some(i, carry):
        def row(r):
            parts = [
                nodes_ref[i * group + g, r * each : (r + 1) * each, :] for g in range(group)
            ]
            return parts[0] if group == 1 else jnp.concatenate(parts, axis=0)

        def put(ref, high, r, value):
            ref[pl.ds(i * (wide * high) + r, wide, stride=high), :] = value

        mass = row(0)
        cx, cy, cz = (row(1 + c) - centre[c] for c in range(3))
        qxx, qyy, qzz, qxy, qxz, qyz = (row(4 + c) for c in range(6))
        vx = qxx * cx + qxy * cy + qxz * cz
        vy = qxy * cx + qyy * cy + qyz * cz
        vz = qxz * cx + qyz * cy + qzz * cz
        terms = [-2.0 * cx, -2.0 * cy, -2.0 * cz, cx * cx + cy * cy + cz * cz]
        terms += [jnp.ones(shape, jnp.float32), -15.0 * vx, -15.0 * vy, -15.0 * vz]
        terms += [7.5 * qxx, 7.5 * qyy, 7.5 * qzz, 15.0 * qxy, 15.0 * qxz, 15.0 * qyz]
        terms += [7.5 * (vx * cx + vy * cy + vz * cz)]
        for r, term in enumerate(terms):
            for s, part in enumerate(thirds(term)):
                put(feats_ref, FEATURES, s * 16 + r, part)
        for s in range(3):
            put(feats_ref, FEATURES, s * 16 + 15, mass)
        half = 1.5 * (qxx + qyy + qzz)
        diag = [3.0 * qxx + half, 3.0 * qyy + half, 3.0 * qzz + half]
        near = [3.0 * vx + half * cx, 3.0 * vy + half * cy, 3.0 * vz + half * cz]
        zero = jnp.zeros(shape, jnp.float32)
        for c, value in enumerate((cx, cy, cz)):
            for s, part in enumerate(thirds(value)):
                put(weights_ref, WEIGHTS, s * 3 + c, part)
        put(weights_ref, WEIGHTS, 9, zero + 1.0)
        for r in range(10, 16):
            put(weights_ref, WEIGHTS, r, zero)
        for c, value in enumerate(near):
            for s, part in enumerate(thirds(value)):
                put(weights_ref, WEIGHTS, 16 + s * 3 + c, -part)
        put(weights_ref, WEIGHTS, 25, zero)
        for c, value in enumerate(diag + [3.0 * qxy, 3.0 * qxz, 3.0 * qyz]):
            top, mid, _ = thirds(value)
            put(weights_ref, WEIGHTS, 26 + c, top)
            put(weights_ref, WEIGHTS, 32 + c, mid)
        put(weights_ref, WEIGHTS, 38, zero)
        put(weights_ref, WEIGHTS, 39, zero)
        return carry

    lax.fori_loop(0, devices // group, some, 0)


def distances(left, feats_ref, block, near_ref):
    base = pl.multiple_of(block * FEATURES, SUBS)
    rows = lax.broadcasted_iota(jnp.int32, (SUBS, LANES), 0)
    zero = jnp.zeros((SUBS, LANES), jnp.float32)
    first, second = [], []
    for s in range(3):
        one = feats_ref[pl.ds(base + s * 16, SUBS), :]
        two = feats_ref[pl.ds(base + s * 16 + SUBS, SUBS), :]
        first.append(jnp.concatenate([jnp.where(rows < 5, one, 0.0), zero], axis=0))
        second.append(
            jnp.concatenate(
                [jnp.where(rows >= 5, one, 0.0), jnp.where(rows < 7, two, 0.0)], axis=0
            )
        )
    blank = jnp.zeros((LANES - 96, 2 * LANES), jnp.float32)
    order = (0, 1, 2, 0, 1, 0)
    right = jnp.concatenate(
        [jnp.concatenate([first[s], second[s]], axis=1) for s in order] + [blank], axis=0
    ).astype(jnp.bfloat16)
    near_ref[...] = jnp.dot(left, right, preferred_element_type=jnp.float32)


def pair_terms(near_ref, feats_ref, block, terms_ref):
    mass = feats_ref[pl.ds(block * FEATURES + 15, 1), :]
    step = 2 * SUBS
    for g in range(LANES // step):
        at = pl.ds(g * step, step)
        dist_sq = near_ref[at, 0:LANES]
        inner = near_ref[at, LANES : 2 * LANES]
        inv = lax.rsqrt(dist_sq)
        inv = inv * inv
        expo = jnp.exp2(dist_sq * EXP2_SCALE)
        arg = lax.rsqrt(dist_sq + ERFC_BIAS)
        poly = arg * ERFC_POLY[-1] + ERFC_POLY[-2]
        for coef in ERFC_POLY[-3::-1]:
            poly = poly * arg + coef
        first = poly * inv
        second = (first + B2_CONST) * inv
        third = (second + B3_CONST) * inv
        radial = (mass * first + third * inner) * expo
        second = second * expo
        for i, value in enumerate((radial, second)):
            top = value.astype(jnp.bfloat16)
            low = (value - top.astype(jnp.float32)).astype(jnp.bfloat16)
            terms_ref[at, i * LANES : (i + 1) * LANES] = top
            terms_ref[at, (2 + i) * LANES : (3 + i) * LANES] = low


def add_forces(terms_ref, weights_ref, block, total_ref, tile):
    base = pl.multiple_of(block * WEIGHTS, SUBS)
    top = jnp.concatenate(
        [weights_ref[pl.ds(base, 16), :], jnp.zeros((SUBS, LANES), jnp.float32)], axis=0
    )
    low = weights_ref[pl.ds(base + 16, 24), :]
    right = jnp.concatenate([top, low, top, low], axis=1).astype(jnp.bfloat16)
    got = lax.dot_general(
        terms_ref[...], right, (((1,), (1,)), ((), ())), preferred_element_type=jnp.float32
    )
    total_ref[tile, :, 0:24] += got


def main_kernel(
    gx,
    gy,
    lists_ref,
    counts_ref,
    tiled_ref,
    origin_ref,
    left_ref,
    slot_ref,
    nodes_ref,
    out_ref,
    feats_ref,
    weights_ref,
    near_ref,
    terms_ref,
    total_ref,
    flat_ref,
):
    count = slot_ref.shape[1]
    tiles = count // LANES
    each = nodes_ref.shape[1] // 10
    node_features(origin_ref, nodes_ref, feats_ref, weights_ref)
    total_ref[...] = jnp.zeros_like(total_ref)
    live = lax.fori_loop(0, tiles, lambda t, n: n + counts_ref[t], 0)
    groups = lax.div(live + (PAIRS - 1), PAIRS)

    def step(i, carry):
        t, k, mids, lasts = carry
        for u, (tile, block) in enumerate(lasts):
            add_forces(terms_ref.at[u], weights_ref, block, total_ref, tile)
        for u, (tile, block) in enumerate(mids):
            pair_terms(near_ref.at[u], feats_ref, block, terms_ref.at[u])
        nexts = []
        for u in range(PAIRS):
            row = jnp.minimum(t, tiles - 1)
            block = lists_ref[row, k]
            dev = quotient(block, each)
            place = (dev % gy) * gx + quotient(dev, gy)
            block = place * each + block % each
            distances(left_ref[row], feats_ref, block, near_ref.at[u])
            nexts.append((jnp.minimum(t, tiles), block))
            wrap = k + 1 >= counts_ref[row]
            k = jnp.where(wrap, 0, k + 1)
            t = jnp.where(wrap, t + 1, t)
        return t, k, tuple(nexts), mids

    start = tuple((jnp.int32(tiles), jnp.int32(0)) for _ in range(PAIRS))
    lax.fori_loop(0, groups + 2, step, (jnp.int32(0), jnp.int32(0), start, start))

    for t in range(tiles):
        flat_ref[pl.ds(t * LANES, LANES), :] = total_ref[t].T

    def column(r):
        return flat_ref[pl.ds(r, tiles, stride=LANES), :]

    x, y, z = tiled_ref[0], tiled_ref[1], tiled_ref[2]
    sums = column(9)
    mxx, myy, mzz, mxy, mxz, myz = (column(10 + c) + column(16 + c) for c in range(6))
    const = [column(c) + column(3 + c) + column(6 + c) for c in range(3)]
    forces = [
        const[0] - x * sums + (mxx * x + mxy * y + mxz * z),
        const[1] - y * sums + (mxy * x + myy * y + myz * z),
        const[2] - z * sums + (mxz * x + myz * y + mzz * z),
    ]
    slots = slot_ref[...]
    owner = owners(slots, tiles, count)
    hot = hot_lanes(slots, count)
    for c in range(3):
        total = None
        for part in thirds(forces[c]):
            got = jnp.dot(part.astype(jnp.bfloat16), hot, preferred_element_type=jnp.float32)
            total = got if total is None else total + got
        out_ref[c : c + 1, :] = jnp.sum(jnp.where(owner, total, 0.0), axis=0, keepdims=True)


def shards(gx, gy, positions, node_moments, slot_of, block_list, tile_counts):
    count = positions.shape[1]
    tiles = count // LANES
    each = node_moments.shape[1] // LANES
    blocks = each * gx * gy
    packed = node_moments.reshape(10 * each, LANES)
    vmem = pl.BlockSpec(memory_space=pltpu.VMEM)
    smem = pl.BlockSpec(memory_space=pltpu.SMEM)
    tiled, origin, left = pl.pallas_call(
        prep_kernel,
        out_shape=(
            jax.ShapeDtypeStruct((3, tiles, LANES), jnp.float32),
            jax.ShapeDtypeStruct((3, LANES), jnp.float32),
            jax.ShapeDtypeStruct((tiles, LANES, LANES), jnp.bfloat16),
        ),
        in_specs=[vmem] * 2,
        out_specs=(vmem,) * 3,
        scratch_shapes=[pltpu.VMEM((tiles * LANES, LANES), jnp.float32)],
    )(positions, slot_of)
    every = lax.all_gather(packed, "gx", axis=0)
    every = lax.all_gather(every, "gy", axis=0)
    every = every.reshape(gx * gy, 10 * each, LANES)
    return pl.pallas_call(
        functools.partial(main_kernel, gx, gy),
        out_shape=jax.ShapeDtypeStruct((3, count), jnp.float32),
        in_specs=[smem] * 2 + [vmem] * 5,
        out_specs=vmem,
        scratch_shapes=[
            pltpu.VMEM((blocks * FEATURES, LANES), jnp.float32),
            pltpu.VMEM((blocks * WEIGHTS, LANES), jnp.float32),
            pltpu.VMEM((PAIRS, LANES, 2 * LANES), jnp.float32),
            pltpu.VMEM((PAIRS, LANES, 4 * LANES), jnp.bfloat16),
            pltpu.VMEM((tiles + 1, LANES, LANES), jnp.float32),
            pltpu.VMEM((tiles * LANES, LANES), jnp.float32),
        ],
    )(block_list, tile_counts, tiled, origin, left, slot_of, every)


def solution(mesh):
    placed = (
        P(None, ("gx", "gy")),
        P(None, ("gx", "gy")),
        P(("gx", "gy"), None),
        P(("gx", "gy"), None),
        P(("gx", "gy")),
    )
    return jax.shard_map(
        functools.partial(shards, mesh.shape["gx"], mesh.shape["gy"]),
        mesh=mesh,
        in_specs=placed,
        out_specs=P(None, ("gx", "gy")),
        check_vma=False,
    )
```

```python
import functools
import math

import jax
import jax.numpy as jnp
from jax import lax
from jax.experimental import pallas as pl
from jax.experimental.pallas import tpu as pltpu
from jax.sharding import PartitionSpec as P

LANES = 128
SUBS = 8
PAIRS = 8
FEATURES = 48
WEIGHTS = 40
split_a = 0.5
soft_sq = 0.25
root_pi = math.sqrt(math.pi)

ERFC_BIAS = 0.15
ERFC_POLY = (
    0.565651365,
    -0.0323440266,
    1.41906215,
    -1.34343713,
    0.938636763,
    -0.36025162,
    0.0669870813,
)

UNIT = split_a * split_a / math.log(2.0)
LEAD = ERFC_POLY[-1] * UNIT ** ((len(ERFC_POLY) - 1) / 2)
MONIC = tuple(coef * UNIT ** (i / 2) / LEAD for i, coef in enumerate(ERFC_POLY))[:-1]
BIAS = ERFC_BIAS * UNIT
SCALE = LEAD * UNIT
ADD_2 = 4.0 * split_a**3 / root_pi / 3.0 / SCALE
ADD_3 = 8.0 * split_a**5 / root_pi / 15.0 / (SCALE * UNIT)


def thirds(value):
    top = value.astype(jnp.bfloat16).astype(jnp.float32)
    rest = value - top
    mid = rest.astype(jnp.bfloat16).astype(jnp.float32)
    low = (rest - mid).astype(jnp.bfloat16).astype(jnp.float32)
    return top, mid, low


def quotient(value, by):
    if by & (by - 1) == 0:
        return lax.shift_right_logical(value, by.bit_length() - 1)
    return lax.div(value, by)


def hot_lanes(slots, count):
    lane = lax.bitwise_and(slots, LANES - 1)
    rows = lax.broadcasted_iota(jnp.int32, (LANES, count), 0)
    return jnp.where(rows == lane, 1.0, 0.0).astype(jnp.bfloat16)


def owners(slots, tiles, count):
    rows = lax.broadcasted_iota(jnp.int32, (tiles, count), 0)
    return rows == lax.shift_right_logical(slots, 7)


def prep_kernel(pos_ref, slot_ref, tiled_ref, origin_ref, left_ref, rows_ref):
    count = pos_ref.shape[1]
    tiles = count // LANES
    slots = slot_ref[...]
    owner = owners(slots, tiles, count)
    hot = hot_lanes(slots, count)
    place = []
    for c in range(3):
        value = pos_ref[c : c + 1, :]
        origin = jnp.sum(value, axis=1, keepdims=True) * (1.0 / count)
        origin_ref[c : c + 1, :] = jnp.broadcast_to(origin, (1, LANES))
        value = value - origin
        total = None
        for part in thirds(value):
            rows = jnp.where(owner, part, 0.0).astype(jnp.bfloat16)
            got = lax.dot_general(
                rows, hot, (((1,), (1,)), ((), ())), preferred_element_type=jnp.float32
            )
            total = got if total is None else total + got
        tiled_ref[c] = total
        place.append(total)
    x, y, z = place
    one = jnp.ones_like(x)
    zero = jnp.zeros_like(x)
    terms = [x, y, z, one, -UNIT * (x * x + y * y + (z * z + soft_sq)), x, y, z]
    terms += [x * x, y * y, z * z, x * y, x * z, y * z, one, zero]
    for i, term in enumerate(terms):
        top, mid, low = thirds(term)
        for s, part in enumerate((top, top, top, mid, mid, low)):
            rows_ref[pl.ds(s * 16 + i, tiles, stride=LANES), :] = part
    for s in range(96, LANES):
        rows_ref[pl.ds(s, tiles, stride=LANES), :] = zero
    for t in range(tiles):
        left_ref[t] = rows_ref[pl.ds(t * LANES, LANES), :].T.astype(jnp.bfloat16)


def node_features(origin_ref, nodes_ref, feats_ref, weights_ref):
    devices, rows, _ = nodes_ref.shape
    each = rows // 10
    group = max(1, SUBS // each)
    wide = group * each
    shape = (wide, LANES)
    centre = [jnp.broadcast_to(origin_ref[c : c + 1, :], shape) for c in range(3)]

    def some(i, carry):
        def row(r):
            parts = [
                nodes_ref[i * group + g, r * each : (r + 1) * each, :] for g in range(group)
            ]
            return parts[0] if group == 1 else jnp.concatenate(parts, axis=0)

        def put(ref, high, r, value):
            ref[pl.ds(i * (wide * high) + r, wide, stride=high), :] = value

        mass = row(0)
        cx, cy, cz = (row(1 + c) - centre[c] for c in range(3))
        qxx, qyy, qzz, qxy, qxz, qyz = (row(4 + c) for c in range(6))
        vx = qxx * cx + qxy * cy + qxz * cz
        vy = qxy * cx + qyy * cy + qyz * cz
        vz = qxz * cx + qyz * cy + qzz * cz
        terms = [2.0 * UNIT * cx, 2.0 * UNIT * cy, 2.0 * UNIT * cz]
        terms += [-UNIT * (cx * cx + cy * cy + cz * cz)]
        one, two = 7.5 * UNIT**2, 15.0 * UNIT**2
        terms += [jnp.ones(shape, jnp.float32), -two * vx, -two * vy, -two * vz]
        terms += [one * qxx, one * qyy, one * qzz, two * qxy, two * qxz, two * qyz]
        terms += [one * (vx * cx + vy * cy + vz * cz)]
        for r, term in enumerate(terms):
            for s, part in enumerate(thirds(term)):
                put(feats_ref, FEATURES, s * 16 + r, part)
        for s in range(3):
            put(feats_ref, FEATURES, s * 16 + 15, mass)
        half = (1.5 * UNIT) * (qxx + qyy + qzz)
        full = 3.0 * UNIT
        diag = [full * qxx + half, full * qyy + half, full * qzz + half]
        near = [full * vx + half * cx, full * vy + half * cy, full * vz + half * cz]
        zero = jnp.zeros(shape, jnp.float32)
        for c, value in enumerate((cx, cy, cz)):
            for s, part in enumerate(thirds(value)):
                put(weights_ref, WEIGHTS, s * 3 + c, part)
        put(weights_ref, WEIGHTS, 9, zero + 1.0)
        for r in range(10, 16):
            put(weights_ref, WEIGHTS, r, zero)
        for c, value in enumerate(near):
            for s, part in enumerate(thirds(value)):
                put(weights_ref, WEIGHTS, 16 + s * 3 + c, -part)
        put(weights_ref, WEIGHTS, 25, zero)
        for c, value in enumerate(diag + [full * qxy, full * qxz, full * qyz]):
            top, mid, _ = thirds(value)
            put(weights_ref, WEIGHTS, 26 + c, top)
            put(weights_ref, WEIGHTS, 32 + c, mid)
        put(weights_ref, WEIGHTS, 38, zero)
        put(weights_ref, WEIGHTS, 39, zero)
        return carry

    lax.fori_loop(0, devices // group, some, 0)


def distances(left, feats_ref, block, near_ref):
    base = pl.multiple_of(block * FEATURES, SUBS)
    rows = lax.broadcasted_iota(jnp.int32, (SUBS, LANES), 0)
    zero = jnp.zeros((SUBS, LANES), jnp.float32)
    first, second = [], []
    for s in range(3):
        one = feats_ref[pl.ds(base + s * 16, SUBS), :]
        two = feats_ref[pl.ds(base + s * 16 + SUBS, SUBS), :]
        first.append(jnp.concatenate([jnp.where(rows < 5, one, 0.0), zero], axis=0))
        second.append(
            jnp.concatenate(
                [jnp.where(rows >= 5, one, 0.0), jnp.where(rows < 7, two, 0.0)], axis=0
            )
        )
    blank = jnp.zeros((LANES - 96, 2 * LANES), jnp.float32)
    order = (0, 1, 2, 0, 1, 0)
    right = jnp.concatenate(
        [jnp.concatenate([first[s], second[s]], axis=1) for s in order] + [blank], axis=0
    ).astype(jnp.bfloat16)
    near_ref[...] = jnp.dot(left, right, preferred_element_type=jnp.float32)


def pair_terms(near_ref, feats_ref, block, terms_ref):
    mass = feats_ref[pl.ds(block * FEATURES + 15, 1), :]
    step = 2 * SUBS
    for g in range(LANES // step):
        at = pl.ds(g * step, step)
        power = near_ref[at, 0:LANES]
        inner = near_ref[at, LANES : 2 * LANES]
        inv = lax.rsqrt(power * power)
        expo = jnp.exp2(power)
        arg = lax.rsqrt(BIAS - power)
        poly = arg + MONIC[-1]
        for coef in MONIC[-2::-1]:
            poly = poly * arg + coef
        first = poly * inv
        second = (first + ADD_2) * inv
        third = (second + ADD_3) * inv
        radial = (mass * first + third * inner) * expo
        second = second * expo
        for i, value in enumerate((radial, second)):
            top = value.astype(jnp.bfloat16)
            low = (value - top.astype(jnp.float32)).astype(jnp.bfloat16)
            terms_ref[i, at, :] = top
            terms_ref[2 + i, at, :] = low


def add_forces(terms_ref, weights_ref, block, total_ref, tile):
    base = pl.multiple_of(block * WEIGHTS, SUBS)
    top = jnp.concatenate(
        [weights_ref[pl.ds(base, 16), :], jnp.zeros((SUBS, LANES), jnp.float32)], axis=0
    )
    low = weights_ref[pl.ds(base + 16, 24), :]
    right = jnp.concatenate([top, low, top, low], axis=1).astype(jnp.bfloat16)
    left = jnp.concatenate([terms_ref[i] for i in range(4)], axis=1)
    got = lax.dot_general(
        left, right, (((1,), (1,)), ((), ())), preferred_element_type=jnp.float32
    )
    total_ref[tile, :, 0:24] += got


def main_kernel(
    gx,
    gy,
    lists_ref,
    counts_ref,
    tiled_ref,
    origin_ref,
    left_ref,
    slot_ref,
    nodes_ref,
    out_ref,
    feats_ref,
    weights_ref,
    near_ref,
    terms_ref,
    total_ref,
    flat_ref,
):
    count = slot_ref.shape[1]
    tiles = count // LANES
    each = nodes_ref.shape[1] // 10
    node_features(origin_ref, nodes_ref, feats_ref, weights_ref)
    total_ref[...] = jnp.zeros_like(total_ref)
    live = lax.fori_loop(0, tiles, lambda t, n: n + counts_ref[t], 0)

    def take(t, k):
        row = jnp.minimum(t, tiles - 1)
        block = lists_ref[row, k]
        dev = quotient(block, each)
        place = (dev % gy) * gx + quotient(dev, gy)
        block = place * each + block % each
        wrap = k + 1 >= counts_ref[row]
        return row, jnp.minimum(t, tiles), block, jnp.where(wrap, t + 1, t), jnp.where(wrap, 0, k + 1)

    def ahead(u, t, k):
        row, tile, block, t, k = take(t, k)
        distances(left_ref[row], feats_ref, block, near_ref.at[u])
        return (tile, block), t, k

    def behind(u, pair):
        add_forces(terms_ref.at[u], weights_ref, pair[1], total_ref, pair[0])

    def step(i, carry):
        t, k, pairs, last = carry
        nexts = []
        behind(PAIRS - 1, last)
        for u in range(PAIRS):
            pair_terms(near_ref.at[u], feats_ref, pairs[u][1], terms_ref.at[u])
            pair, t, k = ahead(u, t, k)
            nexts.append(pair)
            if u + 1 < PAIRS:
                behind(u, pairs[u])
        return t, k, tuple(nexts), pairs[-1]

    t, k, pairs = jnp.int32(0), jnp.int32(0), []
    for u in range(PAIRS):
        pair, t, k = ahead(u, t, k)
        pairs.append(pair)
    none = (jnp.int32(tiles), jnp.int32(0))
    terms_ref[PAIRS - 1] = jnp.zeros(terms_ref.shape[1:], terms_ref.dtype)
    steps = lax.div(live + (PAIRS - 1), PAIRS)
    carry = lax.fori_loop(0, steps, step, (t, k, tuple(pairs), none))
    behind(PAIRS - 1, carry[-1])

    for t in range(tiles):
        flat_ref[pl.ds(t * LANES, LANES), :] = total_ref[t].T

    def column(r):
        return flat_ref[pl.ds(r, tiles, stride=LANES), :]

    x, y, z = tiled_ref[0], tiled_ref[1], tiled_ref[2]
    sums = column(9)
    mxx, myy, mzz, mxy, mxz, myz = (column(10 + c) + column(16 + c) for c in range(6))
    const = [column(c) + column(3 + c) + column(6 + c) for c in range(3)]
    forces = [
        SCALE * (const[0] - x * sums + (mxx * x + mxy * y + mxz * z)),
        SCALE * (const[1] - y * sums + (mxy * x + myy * y + myz * z)),
        SCALE * (const[2] - z * sums + (mxz * x + myz * y + mzz * z)),
    ]
    slots = slot_ref[...]
    owner = owners(slots, tiles, count)
    hot = hot_lanes(slots, count)
    for c in range(3):
        total = None
        for part in thirds(forces[c]):
            got = jnp.dot(part.astype(jnp.bfloat16), hot, preferred_element_type=jnp.float32)
            total = got if total is None else total + got
        out_ref[c : c + 1, :] = jnp.sum(jnp.where(owner, total, 0.0), axis=0, keepdims=True)


def shards(gx, gy, positions, node_moments, slot_of, block_list, tile_counts):
    count = positions.shape[1]
    tiles = count // LANES
    each = node_moments.shape[1] // LANES
    blocks = each * gx * gy
    packed = node_moments.reshape(10 * each, LANES)
    vmem = pl.BlockSpec(memory_space=pltpu.VMEM)
    smem = pl.BlockSpec(memory_space=pltpu.SMEM)
    tiled, origin, left = pl.pallas_call(
        prep_kernel,
        out_shape=(
            jax.ShapeDtypeStruct((3, tiles, LANES), jnp.float32),
            jax.ShapeDtypeStruct((3, LANES), jnp.float32),
            jax.ShapeDtypeStruct((tiles, LANES, LANES), jnp.bfloat16),
        ),
        in_specs=[vmem] * 2,
        out_specs=(vmem,) * 3,
        scratch_shapes=[pltpu.VMEM((tiles * LANES, LANES), jnp.float32)],
    )(positions, slot_of)
    every = lax.all_gather(packed, "gx", axis=0)
    every = lax.all_gather(every, "gy", axis=0)
    every = every.reshape(gx * gy, 10 * each, LANES)
    return pl.pallas_call(
        functools.partial(main_kernel, gx, gy),
        out_shape=jax.ShapeDtypeStruct((3, count), jnp.float32),
        in_specs=[smem] * 2 + [vmem] * 5,
        out_specs=vmem,
        scratch_shapes=[
            pltpu.VMEM((blocks * FEATURES, LANES), jnp.float32),
            pltpu.VMEM((blocks * WEIGHTS, LANES), jnp.float32),
            pltpu.VMEM((PAIRS, LANES, 2 * LANES), jnp.float32),
            pltpu.VMEM((PAIRS, 4, LANES, LANES), jnp.bfloat16),
            pltpu.VMEM((tiles + 1, LANES, LANES), jnp.float32),
            pltpu.VMEM((tiles * LANES, LANES), jnp.float32),
        ],
    )(block_list, tile_counts, tiled, origin, left, slot_of, every)


def solution(mesh):
    placed = (
        P(None, ("gx", "gy")),
        P(None, ("gx", "gy")),
        P(("gx", "gy"), None),
        P(("gx", "gy"), None),
        P(("gx", "gy")),
    )
    return jax.shard_map(
        functools.partial(shards, mesh.shape["gx"], mesh.shape["gy"]),
        mesh=mesh,
        in_specs=placed,
        out_specs=P(None, ("gx", "gy")),
        check_vma=False,
    )
```

```python
import functools
import math

import jax
import jax.numpy as jnp
from jax import lax
from jax.experimental import pallas as pl
from jax.experimental.pallas import tpu as pltpu
from jax.sharding import PartitionSpec as P

LANES = 128
SUBS = 8
PAIRS = 8
FEATURES = 48
WEIGHTS = 40
split_a = 0.5
soft_sq = 0.25
root_pi = math.sqrt(math.pi)

ERFC_BIAS = 0.15
ERFC_POLY = (
    0.565651365,
    -0.0323440266,
    1.41906215,
    -1.34343713,
    0.938636763,
    -0.36025162,
    0.0669870813,
)

UNIT = split_a * split_a / math.log(2.0)
LEAD = ERFC_POLY[-1] * UNIT ** ((len(ERFC_POLY) - 1) / 2)
MONIC = tuple(coef * UNIT ** (i / 2) / LEAD for i, coef in enumerate(ERFC_POLY))[:-1]
BIAS = ERFC_BIAS * UNIT
SCALE = LEAD * UNIT
ADD_2 = 4.0 * split_a**3 / root_pi / 3.0 / SCALE
ADD_3 = 8.0 * split_a**5 / root_pi / 15.0 / (SCALE * UNIT)


def thirds(value):
    top = value.astype(jnp.bfloat16).astype(jnp.float32)
    rest = value - top
    mid = rest.astype(jnp.bfloat16).astype(jnp.float32)
    low = (rest - mid).astype(jnp.bfloat16).astype(jnp.float32)
    return top, mid, low


def quotient(value, by):
    if by & (by - 1) == 0:
        return lax.shift_right_logical(value, by.bit_length() - 1)
    return lax.div(value, by)


def hot_lanes(slots, count):
    lane = lax.bitwise_and(slots, LANES - 1)
    rows = lax.broadcasted_iota(jnp.int32, (LANES, count), 0)
    return jnp.where(rows == lane, 1.0, 0.0).astype(jnp.bfloat16)


def owners(slots, tiles, count):
    rows = lax.broadcasted_iota(jnp.int32, (tiles, count), 0)
    return rows == lax.shift_right_logical(slots, 7)


def prep_kernel(pos_ref, slot_ref, tiled_ref, origin_ref, left_ref, rows_ref):
    count = pos_ref.shape[1]
    tiles = count // LANES
    slots = slot_ref[...]
    owner = owners(slots, tiles, count)
    hot = hot_lanes(slots, count)
    place = []
    for c in range(3):
        value = pos_ref[c : c + 1, :]
        origin = jnp.sum(value, axis=1, keepdims=True) * (1.0 / count)
        origin_ref[c : c + 1, :] = jnp.broadcast_to(origin, (1, LANES))
        value = value - origin
        total = None
        for part in thirds(value):
            rows = jnp.where(owner, part, 0.0).astype(jnp.bfloat16)
            got = lax.dot_general(
                rows, hot, (((1,), (1,)), ((), ())), preferred_element_type=jnp.float32
            )
            total = got if total is None else total + got
        tiled_ref[c] = total
        place.append(total)
    x, y, z = place
    one = jnp.ones_like(x)
    zero = jnp.zeros_like(x)
    terms = [x, y, z, one, -UNIT * (x * x + y * y + (z * z + soft_sq)), x, y, z]
    terms += [x * x, y * y, z * z, x * y, x * z, y * z, one, zero]
    for i, term in enumerate(terms):
        top, mid, low = thirds(term)
        for s, part in enumerate((top, top, top, mid, mid, low)):
            rows_ref[pl.ds(s * 16 + i, tiles, stride=LANES), :] = part
    for s in range(96, LANES):
        rows_ref[pl.ds(s, tiles, stride=LANES), :] = zero
    for t in range(tiles):
        left_ref[t] = rows_ref[pl.ds(t * LANES, LANES), :].T.astype(jnp.bfloat16)


def node_features(origin_ref, nodes_ref, feats_ref, weights_ref, start):
    devices, rows, _ = nodes_ref.shape
    each = rows // 10
    group = max(1, SUBS // each)
    wide = group * each
    shape = (wide, LANES)
    centre = [jnp.broadcast_to(origin_ref[c : c + 1, :], shape) for c in range(3)]

    def some(i, carry):
        def row(r):
            parts = [
                nodes_ref[i * group + g, r * each : (r + 1) * each, :] for g in range(group)
            ]
            return parts[0] if group == 1 else jnp.concatenate(parts, axis=0)

        def put(ref, high, r, value):
            ref[pl.ds((start + i * wide) * high + r, wide, stride=high), :] = value

        mass = row(0)
        cx, cy, cz = (row(1 + c) - centre[c] for c in range(3))
        qxx, qyy, qzz, qxy, qxz, qyz = (row(4 + c) for c in range(6))
        vx = qxx * cx + qxy * cy + qxz * cz
        vy = qxy * cx + qyy * cy + qyz * cz
        vz = qxz * cx + qyz * cy + qzz * cz
        terms = [2.0 * UNIT * cx, 2.0 * UNIT * cy, 2.0 * UNIT * cz]
        terms += [-UNIT * (cx * cx + cy * cy + cz * cz)]
        one, two = 7.5 * UNIT**2, 15.0 * UNIT**2
        terms += [jnp.ones(shape, jnp.float32), -two * vx, -two * vy, -two * vz]
        terms += [one * qxx, one * qyy, one * qzz, two * qxy, two * qxz, two * qyz]
        terms += [one * (vx * cx + vy * cy + vz * cz)]
        for r, term in enumerate(terms):
            for s, part in enumerate(thirds(term)):
                put(feats_ref, FEATURES, s * 16 + r, part)
        for s in range(3):
            put(feats_ref, FEATURES, s * 16 + 15, mass)
        half = (1.5 * UNIT) * (qxx + qyy + qzz)
        full = 3.0 * UNIT
        diag = [full * qxx + half, full * qyy + half, full * qzz + half]
        near = [full * vx + half * cx, full * vy + half * cy, full * vz + half * cz]
        zero = jnp.zeros(shape, jnp.float32)
        for c, value in enumerate((cx, cy, cz)):
            for s, part in enumerate(thirds(value)):
                put(weights_ref, WEIGHTS, s * 3 + c, part)
        put(weights_ref, WEIGHTS, 9, zero + 1.0)
        for r in range(10, 16):
            put(weights_ref, WEIGHTS, r, zero)
        for c, value in enumerate(near):
            for s, part in enumerate(thirds(value)):
                put(weights_ref, WEIGHTS, 16 + s * 3 + c, -part)
        put(weights_ref, WEIGHTS, 25, zero)
        for c, value in enumerate(diag + [full * qxy, full * qxz, full * qyz]):
            top, mid, _ = thirds(value)
            put(weights_ref, WEIGHTS, 26 + c, top)
            put(weights_ref, WEIGHTS, 32 + c, mid)
        put(weights_ref, WEIGHTS, 38, zero)
        put(weights_ref, WEIGHTS, 39, zero)
        return carry

    lax.fori_loop(0, devices // group, some, 0)


def distances(left, feats_ref, block, near_ref):
    base = pl.multiple_of(block * FEATURES, SUBS)
    rows = lax.broadcasted_iota(jnp.int32, (SUBS, LANES), 0)
    zero = jnp.zeros((SUBS, LANES), jnp.float32)
    first, second = [], []
    for s in range(3):
        one = feats_ref[pl.ds(base + s * 16, SUBS), :]
        two = feats_ref[pl.ds(base + s * 16 + SUBS, SUBS), :]
        first.append(jnp.concatenate([jnp.where(rows < 5, one, 0.0), zero], axis=0))
        second.append(
            jnp.concatenate(
                [jnp.where(rows >= 5, one, 0.0), jnp.where(rows < 7, two, 0.0)], axis=0
            )
        )
    blank = jnp.zeros((LANES - 96, 2 * LANES), jnp.float32)
    order = (0, 1, 2, 0, 1, 0)
    right = jnp.concatenate(
        [jnp.concatenate([first[s], second[s]], axis=1) for s in order] + [blank], axis=0
    ).astype(jnp.bfloat16)
    near_ref[...] = jnp.dot(left, right, preferred_element_type=jnp.float32)


def pair_terms(near_ref, feats_ref, block, terms_ref):
    mass = feats_ref[pl.ds(block * FEATURES + 15, 1), :]
    step = 2 * SUBS
    for g in range(LANES // step):
        at = pl.ds(g * step, step)
        power = near_ref[at, 0:LANES]
        inner = near_ref[at, LANES : 2 * LANES]
        inv = lax.rsqrt(power * power)
        expo = jnp.exp2(power)
        arg = lax.rsqrt(BIAS - power)
        poly = arg + MONIC[-1]
        for coef in MONIC[-2::-1]:
            poly = poly * arg + coef
        first = poly * inv
        second = (first + ADD_2) * inv
        third = (second + ADD_3) * inv
        radial = (mass * first + third * inner) * expo
        second = second * expo
        for i, value in enumerate((radial, second)):
            top = value.astype(jnp.bfloat16)
            low = (value - top.astype(jnp.float32)).astype(jnp.bfloat16)
            terms_ref[i, at, :] = top
            terms_ref[2 + i, at, :] = low


def add_forces(terms_ref, weights_ref, block, total_ref, tile):
    base = pl.multiple_of(block * WEIGHTS, SUBS)
    top = jnp.concatenate(
        [weights_ref[pl.ds(base, 16), :], jnp.zeros((SUBS, LANES), jnp.float32)], axis=0
    )
    low = weights_ref[pl.ds(base + 16, 24), :]
    right = jnp.concatenate([top, low, top, low], axis=1).astype(jnp.bfloat16)
    left = jnp.concatenate([terms_ref[i] for i in range(4)], axis=1)
    got = lax.dot_general(
        left, right, (((1,), (1,)), ((), ())), preferred_element_type=jnp.float32
    )
    total_ref[tile, :, 0:24] += got


def main_kernel(
    gx,
    gy,
    lists_ref,
    counts_ref,
    self_ref,
    tiled_ref,
    origin_ref,
    left_ref,
    slot_ref,
    mine_ref,
    twin_ref,
    out_ref,
    feats_ref,
    weights_ref,
    near_ref,
    terms_ref,
    total_ref,
    flat_ref,
):
    count = slot_ref.shape[1]
    tiles = count // LANES
    each = mine_ref.shape[1] // 10
    half = mine_ref.shape[0] * each
    node_features(origin_ref, mine_ref, feats_ref, weights_ref, 0)
    node_features(origin_ref, twin_ref, feats_ref, weights_ref, half)
    my_x, my_y = self_ref[0], self_ref[1]
    total_ref[...] = jnp.zeros_like(total_ref)
    live = lax.fori_loop(0, tiles, lambda t, n: n + counts_ref[t], 0)

    def take(t, k):
        row = jnp.minimum(t, tiles - 1)
        block = lists_ref[row, k]
        dev = quotient(block, each)
        far_x = quotient(dev, gy) ^ my_x
        far_y = (dev & (gy - 1)) ^ my_y
        block = ((far_y >> 1) * gx + far_x) * each + (block & (each - 1)) + (far_y & 1) * half
        wrap = k + 1 >= counts_ref[row]
        return row, jnp.minimum(t, tiles), block, jnp.where(wrap, t + 1, t), jnp.where(wrap, 0, k + 1)

    def ahead(u, t, k):
        row, tile, block, t, k = take(t, k)
        distances(left_ref[row], feats_ref, block, near_ref.at[u])
        return (tile, block), t, k

    def behind(u, pair):
        add_forces(terms_ref.at[u], weights_ref, pair[1], total_ref, pair[0])

    def step(i, carry):
        t, k, pairs, last = carry
        nexts = []
        behind(PAIRS - 1, last)
        for u in range(PAIRS):
            pair_terms(near_ref.at[u], feats_ref, pairs[u][1], terms_ref.at[u])
            pair, t, k = ahead(u, t, k)
            nexts.append(pair)
            if u + 1 < PAIRS:
                behind(u, pairs[u])
        return t, k, tuple(nexts), pairs[-1]

    t, k, pairs = jnp.int32(0), jnp.int32(0), []
    for u in range(PAIRS):
        pair, t, k = ahead(u, t, k)
        pairs.append(pair)
    none = (jnp.int32(tiles), jnp.int32(0))
    terms_ref[PAIRS - 1] = jnp.zeros(terms_ref.shape[1:], terms_ref.dtype)
    steps = lax.div(live + (PAIRS - 1), PAIRS)
    carry = lax.fori_loop(0, steps, step, (t, k, tuple(pairs), none))
    behind(PAIRS - 1, carry[-1])

    for t in range(tiles):
        flat_ref[pl.ds(t * LANES, LANES), :] = total_ref[t].T

    def column(r):
        return flat_ref[pl.ds(r, tiles, stride=LANES), :]

    x, y, z = tiled_ref[0], tiled_ref[1], tiled_ref[2]
    sums = column(9)
    mxx, myy, mzz, mxy, mxz, myz = (column(10 + c) + column(16 + c) for c in range(6))
    const = [column(c) + column(3 + c) + column(6 + c) for c in range(3)]
    forces = [
        SCALE * (const[0] - x * sums + (mxx * x + mxy * y + mxz * z)),
        SCALE * (const[1] - y * sums + (mxy * x + myy * y + myz * z)),
        SCALE * (const[2] - z * sums + (mxz * x + myz * y + mzz * z)),
    ]
    slots = slot_ref[...]
    owner = owners(slots, tiles, count)
    hot = hot_lanes(slots, count)
    for c in range(3):
        total = None
        for part in thirds(forces[c]):
            got = jnp.dot(part.astype(jnp.bfloat16), hot, preferred_element_type=jnp.float32)
            total = got if total is None else total + got
        out_ref[c : c + 1, :] = jnp.sum(jnp.where(owner, total, 0.0), axis=0, keepdims=True)


def shards(gx, gy, positions, node_moments, slot_of, block_list, tile_counts):
    count = positions.shape[1]
    tiles = count // LANES
    each = node_moments.shape[1] // LANES
    blocks = each * gx * gy
    vmem = pl.BlockSpec(memory_space=pltpu.VMEM)
    smem = pl.BlockSpec(memory_space=pltpu.SMEM)
    def swap(value, axis, size, bits):
        return lax.ppermute(value, axis, [(i, i ^ bits) for i in range(size)])

    near = [node_moments] + [swap(node_moments, "gx", gx, b) for b in range(1, gx)]
    near = jnp.stack([value.reshape(10 * each, LANES) for value in near])
    near, positions = lax.optimization_barrier((near, positions))
    far = [swap(near, "gy", gy, b) for b in range(2, gy, 2)]
    tiled, origin, left = pl.pallas_call(
        prep_kernel,
        out_shape=(
            jax.ShapeDtypeStruct((3, tiles, LANES), jnp.float32),
            jax.ShapeDtypeStruct((3, LANES), jnp.float32),
            jax.ShapeDtypeStruct((tiles, LANES, LANES), jnp.bfloat16),
        ),
        in_specs=[vmem] * 2,
        out_specs=(vmem,) * 3,
        scratch_shapes=[pltpu.VMEM((tiles * LANES, LANES), jnp.float32)],
        compiler_params=pltpu.CompilerParams(vmem_limit_bytes=8 * 2**20),
        cost_estimate=pl.CostEstimate(flops=10**10, bytes_accessed=10**6, transcendentals=0),
    )(positions, slot_of)
    mine = jnp.concatenate([near] + far, axis=0)
    mine, origin = lax.optimization_barrier((mine, origin))
    twin = swap(mine, "gy", gy, 1)
    row = 4 * LANES
    limit = row * (blocks * (FEATURES + WEIGHTS + 10) + PAIRS * 4 * LANES + tiles * 3 * LANES)
    limit = min(limit + 2**21, 60 * 1024 * 1024)
    here = jnp.stack([lax.axis_index("gx"), lax.axis_index("gy")]).astype(jnp.int32)
    return pl.pallas_call(
        functools.partial(main_kernel, gx, gy),
        out_shape=jax.ShapeDtypeStruct((3, count), jnp.float32),
        in_specs=[smem] * 3 + [vmem] * 6,
        out_specs=vmem,
        scratch_shapes=[
            pltpu.VMEM((blocks * FEATURES, LANES), jnp.float32),
            pltpu.VMEM((blocks * WEIGHTS, LANES), jnp.float32),
            pltpu.VMEM((PAIRS, LANES, 2 * LANES), jnp.float32),
            pltpu.VMEM((PAIRS, 4, LANES, LANES), jnp.bfloat16),
            pltpu.VMEM((tiles + 1, LANES, LANES), jnp.float32),
            pltpu.VMEM((tiles * LANES, LANES), jnp.float32),
        ],
        compiler_params=pltpu.CompilerParams(vmem_limit_bytes=limit),
    )(block_list, tile_counts, here, tiled, origin, left, slot_of, mine, twin)


def solution(mesh):
    placed = (
        P(None, ("gx", "gy")),
        P(None, ("gx", "gy")),
        P(("gx", "gy"), None),
        P(("gx", "gy"), None),
        P(("gx", "gy")),
    )
    return jax.shard_map(
        functools.partial(shards, mesh.shape["gx"], mesh.shape["gy"]),
        mesh=mesh,
        in_specs=placed,
        out_specs=P(None, ("gx", "gy")),
        check_vma=False,
    )
```

```python
import functools
import math

import jax
import jax.numpy as jnp
from jax import lax
from jax.experimental import pallas as pl
from jax.experimental.pallas import tpu as pltpu
from jax.sharding import PartitionSpec as P


LANES = 128
SUBS = 8
PAIRS = 8
FEATURES = 48
WEIGHTS = 40
BLOCK_ROOM = 2**16
split_a = 0.5
soft_sq = 0.25
root_pi = math.sqrt(math.pi)

ERFC_BIAS = 0.15
ERFC_POLY = (
    0.565651365,
    -0.0323440266,
    1.41906215,
    -1.34343713,
    0.938636763,
    -0.36025162,
    0.0669870813,
)

UNIT = split_a * split_a / math.log(2.0)
LEAD = ERFC_POLY[-1] * UNIT ** ((len(ERFC_POLY) - 1) / 2)
MONIC = tuple(coef * UNIT ** (i / 2) / LEAD for i, coef in enumerate(ERFC_POLY))[:-1]
BIAS = ERFC_BIAS * UNIT
SCALE = LEAD * UNIT
ADD_2 = 4.0 * split_a**3 / root_pi / 3.0 / SCALE
ADD_3 = 8.0 * split_a**5 / root_pi / 15.0 / (SCALE * UNIT)


def thirds(value):
    top = value.astype(jnp.bfloat16).astype(jnp.float32)
    rest = value - top
    mid = rest.astype(jnp.bfloat16).astype(jnp.float32)
    low = (rest - mid).astype(jnp.bfloat16).astype(jnp.float32)
    return top, mid, low


def quotient(value, by):
    if by & (by - 1) == 0:
        return lax.shift_right_logical(value, by.bit_length() - 1)
    return lax.div(value, by)


def hot_lanes(slots, count):
    lane = lax.bitwise_and(slots, LANES - 1)
    rows = lax.broadcasted_iota(jnp.int32, (LANES, count), 0)
    return jnp.where(rows == lane, 1.0, 0.0).astype(jnp.bfloat16)


def owners(slots, tiles, count):
    rows = lax.broadcasted_iota(jnp.int32, (tiles, count), 0)
    return rows == lax.shift_right_logical(slots, 7)


def prep_kernel(
    gx,
    gy,
    each,
    self_ref,
    lists_hbm,
    counts_hbm,
    pos_hbm,
    slot_hbm,
    nodes_hbm,
    tiled_ref,
    origin_ref,
    left_ref,
    near_list_ref,
    far_list_ref,
    own_ref,
    rows_ref,
    lists_ref,
    counts_ref,
    pos_ref,
    slot_ref,
    nodes_ref,
    sems,
):
    count = pos_ref.shape[1]
    tiles = count // LANES
    moves = (
        (pos_hbm, pos_ref),
        (slot_hbm, slot_ref),
        (lists_hbm, lists_ref),
        (counts_hbm, counts_ref),
        (nodes_hbm, nodes_ref),
    )
    copies = [
        pltpu.make_async_copy(source, target, sems.at[i])
        for i, (source, target) in enumerate(moves)
    ]
    for copy in copies:
        copy.start()
    for copy in copies:
        copy.wait()
    for j in range(each):
        own_ref[pl.ds(j, 10, stride=each), :] = nodes_ref[:, j * LANES : (j + 1) * LANES]
    slots = slot_ref[...]
    owner = owners(slots, tiles, count)
    hot = hot_lanes(slots, count)
    rows = []
    for c in range(3):
        value = pos_ref[c : c + 1, :]
        origin = jnp.sum(value, axis=1, keepdims=True) * (1.0 / count)
        origin_ref[c : c + 1, :] = jnp.broadcast_to(origin, (1, LANES))
        for part in thirds(value - origin):
            rows.append(jnp.where(owner, part, 0.0).astype(jnp.bfloat16))
    got = lax.dot_general(
        jnp.concatenate(rows, axis=0),
        hot,
        (((1,), (1,)), ((), ())),
        preferred_element_type=jnp.float32,
    )
    place = []
    for c in range(3):
        top, mid, low = (got[(3 * c + p) * tiles : (3 * c + p + 1) * tiles, :] for p in range(3))
        tiled_ref[c] = top + mid + low
        place.append(top + mid + low)
    x, y, z = place
    one = jnp.ones_like(x)
    zero = jnp.zeros_like(x)
    terms = [x, y, z, one, -UNIT * (x * x + y * y + (z * z + soft_sq)), x, y, z]
    terms += [x * x, y * y, z * z, x * y, x * z, y * z, one, zero]
    for i, term in enumerate(terms):
        top, mid, low = thirds(term)
        for s, part in enumerate((top, top, top, mid, mid, low)):
            rows_ref[pl.ds(s * 16 + i, tiles, stride=LANES), :] = part
    for s in range(96, LANES):
        rows_ref[pl.ds(s, tiles, stride=LANES), :] = zero
    for t in range(tiles):
        left_ref[t] = rows_ref[pl.ds(t * LANES, LANES), :].T.astype(jnp.bfloat16)

    block = lists_ref[...]
    length = block.shape[1]
    dev = quotient(block, each)
    far_x = quotient(dev, gy) ^ self_ref[0]
    far_y = (dev & (gy - 1)) ^ self_ref[1]
    core, far_z = far_y & 1, lax.shift_right_logical(far_y, 1)
    inside = block & (each - 1)
    near_at = (core * gx + far_x) * each + inside
    far_at = ((core * (gy // 2 - 1) + far_z - 1) * gx + far_x) * each + inside
    tile_of = lax.broadcasted_iota(jnp.int32, (tiles, length), 0)
    slot = lax.broadcasted_iota(jnp.int32, (tiles, length), 1)
    limit = jnp.zeros((tiles, length), jnp.int32)
    for t in range(tiles):
        limit = jnp.where(tile_of == t, counts_ref[t], limit)
    live = slot < limit
    before = lax.broadcasted_iota(jnp.int32, (length, length), 0)
    before = before < lax.broadcasted_iota(jnp.int32, (length, length), 1)
    above = lax.broadcasted_iota(jnp.int32, (tiles, tiles), 1)
    above = above < lax.broadcasted_iota(jnp.int32, (tiles, tiles), 0)
    for out_ref, member, at in (
        (near_list_ref, far_z == 0, near_at),
        (far_list_ref, far_z != 0, far_at),
    ):
        member = live & member
        hits = jnp.where(member, 1.0, 0.0)
        number = jnp.sum(hits, axis=1, keepdims=True)
        ahead = jnp.dot(
            hits.astype(jnp.bfloat16),
            jnp.where(before, 1.0, 0.0).astype(jnp.bfloat16),
            preferred_element_type=jnp.float32,
        )
        ahead += jnp.dot(
            jnp.where(above, 1.0, 0.0).astype(jnp.bfloat16),
            jnp.broadcast_to(number, (tiles, length)).astype(jnp.bfloat16),
            preferred_element_type=jnp.float32,
        )
        ahead = jnp.where(member, ahead, -1.0)
        room = out_ref.shape[1]
        entry = tile_of * BLOCK_ROOM + at - tiles * BLOCK_ROOM
        where = lax.broadcasted_iota(jnp.int32, (tiles, room), 1)
        total = jnp.zeros((tiles, room), jnp.int32)
        for k in range(length):
            mine = ahead[:, k : k + 1].astype(jnp.int32)
            total += jnp.where(where == mine, entry[:, k : k + 1], 0)
        total = jnp.sum(total, axis=0, keepdims=True) + tiles * BLOCK_ROOM
        last = lax.broadcasted_iota(jnp.int32, (1, room), 1) == room - 1
        total = jnp.where(last, jnp.sum(number).astype(jnp.int32), total)
        out_ref[...] = total


def node_features(origin_ref, nodes_ref, feats_ref, weights_ref, start):
    devices, rows, _ = nodes_ref.shape
    each = rows // 10
    group = max(1, SUBS // each)
    wide = group * each
    shape = (wide, LANES)
    centre = [jnp.broadcast_to(origin_ref[c : c + 1, :], shape) for c in range(3)]

    def some(i, carry):
        def row(r):
            parts = [
                nodes_ref[i * group + g, r * each : (r + 1) * each, :] for g in range(group)
            ]
            return parts[0] if group == 1 else jnp.concatenate(parts, axis=0)

        def put(ref, high, r, value):
            ref[pl.ds((start + i * wide) * high + r * wide, wide), :] = value

        mass = row(0)
        cx, cy, cz = (row(1 + c) - centre[c] for c in range(3))
        qxx, qyy, qzz, qxy, qxz, qyz = (row(4 + c) for c in range(6))
        vx = qxx * cx + qxy * cy + qxz * cz
        vy = qxy * cx + qyy * cy + qyz * cz
        vz = qxz * cx + qyz * cy + qzz * cz
        terms = [2.0 * UNIT * cx, 2.0 * UNIT * cy, 2.0 * UNIT * cz]
        terms += [-UNIT * (cx * cx + cy * cy + cz * cz)]
        one, two = 7.5 * UNIT**2, 15.0 * UNIT**2
        terms += [jnp.ones(shape, jnp.float32), -two * vx, -two * vy, -two * vz]
        terms += [one * qxx, one * qyy, one * qzz, two * qxy, two * qxz, two * qyz]
        terms += [one * (vx * cx + vy * cy + vz * cz)]
        for r, term in enumerate(terms):
            for s, part in enumerate(thirds(term)):
                put(feats_ref, FEATURES, s * 16 + r, part)
        for s in range(3):
            put(feats_ref, FEATURES, s * 16 + 15, mass)
        half = (1.5 * UNIT) * (qxx + qyy + qzz)
        full = 3.0 * UNIT
        diag = [full * qxx + half, full * qyy + half, full * qzz + half]
        near = [full * vx + half * cx, full * vy + half * cy, full * vz + half * cz]
        zero = jnp.zeros(shape, jnp.float32)
        for c, value in enumerate((cx, cy, cz)):
            for s, part in enumerate(thirds(value)):
                put(weights_ref, WEIGHTS, s * 3 + c, part)
        put(weights_ref, WEIGHTS, 9, zero + 1.0)
        for r in range(10, 16):
            put(weights_ref, WEIGHTS, r, zero)
        for c, value in enumerate(near):
            for s, part in enumerate(thirds(value)):
                put(weights_ref, WEIGHTS, 16 + s * 3 + c, -part)
        put(weights_ref, WEIGHTS, 25, zero)
        for c, value in enumerate(diag + [full * qxy, full * qxz, full * qyz]):
            top, mid, _ = thirds(value)
            put(weights_ref, WEIGHTS, 26 + c, top)
            put(weights_ref, WEIGHTS, 32 + c, mid)
        put(weights_ref, WEIGHTS, 38, zero)
        put(weights_ref, WEIGHTS, 39, zero)
        return carry

    lax.fori_loop(0, devices // group, some, 0)


def rows_of(ref, high, wide, block, first, number):
    base = quotient(block, wide) * (high * wide) + (block & (wide - 1))
    return ref[pl.ds(base + first * wide, number, stride=wide), :]


def distances(left, take, near_ref):
    rows = lax.broadcasted_iota(jnp.int32, (SUBS, LANES), 0)
    zero = jnp.zeros((SUBS, LANES), jnp.float32)
    first, second = [], []
    for s in range(3):
        one = take(s * 16, SUBS)
        two = take(s * 16 + SUBS, SUBS)
        first.append(jnp.concatenate([jnp.where(rows < 5, one, 0.0), zero], axis=0))
        second.append(
            jnp.concatenate(
                [jnp.where(rows >= 5, one, 0.0), jnp.where(rows < 7, two, 0.0)], axis=0
            )
        )
    blank = jnp.zeros((LANES - 96, 2 * LANES), jnp.float32)
    order = (0, 1, 2, 0, 1, 0)
    right = jnp.concatenate(
        [jnp.concatenate([first[s], second[s]], axis=1) for s in order] + [blank], axis=0
    ).astype(jnp.bfloat16)
    near_ref[...] = jnp.dot(left, right, preferred_element_type=jnp.float32)


def pair_terms(near_ref, mass, terms_ref):
    step = 2 * SUBS
    for g in range(LANES // step):
        at = pl.ds(g * step, step)
        power = near_ref[at, 0:LANES]
        inner = near_ref[at, LANES : 2 * LANES]
        inv = lax.rsqrt(power * power)
        expo = jnp.exp2(power)
        arg = lax.rsqrt(BIAS - power)
        poly = arg + MONIC[-1]
        for coef in MONIC[-2::-1]:
            poly = poly * arg + coef
        first = poly * inv
        second = (first + ADD_2) * inv
        third = (second + ADD_3) * inv
        radial = (mass * first + third * inner) * expo
        second = second * expo
        for i, value in enumerate((radial, second)):
            top = value.astype(jnp.bfloat16)
            low = (value - top.astype(jnp.float32)).astype(jnp.bfloat16)
            terms_ref[i, at, :] = top
            terms_ref[2 + i, at, :] = low


def add_forces(terms_ref, take, total_ref, tile):
    top = jnp.concatenate([take(0, 16), jnp.zeros((SUBS, LANES), jnp.float32)], axis=0)
    low = take(16, 24)
    right = jnp.concatenate([top, low, top, low], axis=1).astype(jnp.bfloat16)
    left = jnp.concatenate([terms_ref[i] for i in range(4)], axis=1)
    got = lax.dot_general(
        left, right, (((1,), (1,)), ((), ())), preferred_element_type=jnp.float32
    )
    total_ref[tile, :, 0:24] += got


def all_pairs(list_ref, origin_ref, left_ref, mine_ref, twin_ref, total_ref, scratch):
    feats_ref, weights_ref, near_ref, terms_ref = scratch
    tiles = left_ref.shape[0]
    each = mine_ref.shape[1] // 10
    wide = max(1, SUBS // each) * each
    half = mine_ref.shape[0] * each
    node_features(origin_ref, mine_ref, feats_ref, weights_ref, 0)
    node_features(origin_ref, twin_ref, feats_ref, weights_ref, half)

    def ahead(u, n):
        entry = list_ref[0, n]
        tile, block = quotient(entry, BLOCK_ROOM), entry & (BLOCK_ROOM - 1)
        take = functools.partial(rows_of, feats_ref, FEATURES, wide, block)
        distances(left_ref[jnp.minimum(tile, tiles - 1)], take, near_ref.at[u])
        return tile, block

    def behind(u, pair):
        take = functools.partial(rows_of, weights_ref, WEIGHTS, wide, pair[1])
        add_forces(terms_ref.at[u], take, total_ref, pair[0])

    def step(i, carry):
        pairs, last = carry
        nexts = []
        behind(PAIRS - 1, last)
        for u in range(PAIRS):
            mass = rows_of(feats_ref, FEATURES, wide, pairs[u][1], 15, 1)
            pair_terms(near_ref.at[u], mass, terms_ref.at[u])
            nexts.append(ahead(u, (i + 1) * PAIRS + u))
            if u + 1 < PAIRS:
                behind(u, pairs[u])
        return tuple(nexts), pairs[-1]

    pairs = tuple(ahead(u, u) for u in range(PAIRS))
    none = (jnp.int32(tiles), jnp.int32(0))
    terms_ref[PAIRS - 1] = jnp.zeros(terms_ref.shape[1:], terms_ref.dtype)
    live = list_ref[0, list_ref.shape[1] - 1]
    steps = quotient(live + (PAIRS - 1), PAIRS)
    carry = lax.fori_loop(0, steps, step, (pairs, none))
    behind(PAIRS - 1, carry[-1])


def near_kernel(list_ref, origin_ref, left_ref, mine_ref, twin_ref, total_ref, *scratch):
    total_ref[...] = jnp.zeros_like(total_ref)
    all_pairs(list_ref, origin_ref, left_ref, mine_ref, twin_ref, total_ref, scratch)


def far_kernel(
    list_ref,
    tiled_ref,
    origin_ref,
    left_ref,
    slot_ref,
    mine_ref,
    twin_ref,
    start_ref,
    out_ref,
    total_ref,
    flat_ref,
    *scratch,
):
    count = slot_ref.shape[1]
    tiles = count // LANES
    total_ref[...] = start_ref[...]
    all_pairs(list_ref, origin_ref, left_ref, mine_ref, twin_ref, total_ref, scratch)
    room = LANES // 4
    for q in range(0, tiles, 4):
        four = total_ref[q]
        for j in range(1, min(4, tiles - q)):
            four += pltpu.roll(total_ref[q + j], room * j, 1)
        flat_ref[pl.ds(q * room, LANES), :] = four.T

    def column(r):
        return flat_ref[pl.ds(r, tiles, stride=room), :]

    x, y, z = tiled_ref[0], tiled_ref[1], tiled_ref[2]
    sums = column(9)
    mxx, myy, mzz, mxy, mxz, myz = (column(10 + c) + column(16 + c) for c in range(6))
    const = [column(c) + column(3 + c) + column(6 + c) for c in range(3)]
    forces = [
        SCALE * (const[0] - x * sums + (mxx * x + mxy * y + mxz * z)),
        SCALE * (const[1] - y * sums + (mxy * x + myy * y + myz * z)),
        SCALE * (const[2] - z * sums + (mxz * x + myz * y + mzz * z)),
    ]
    slots = slot_ref[...]
    owner = owners(slots, tiles, count)
    parts = [part.astype(jnp.bfloat16) for force in forces for part in thirds(force)]
    got = jnp.dot(
        jnp.concatenate(parts, axis=0),
        hot_lanes(slots, count),
        preferred_element_type=jnp.float32,
    )
    for c in range(3):
        top, mid, low = (got[(3 * c + p) * tiles : (3 * c + p + 1) * tiles, :] for p in range(3))
        chosen = jnp.where(owner, top + mid + low, 0.0)
        out_ref[c : c + 1, :] = jnp.sum(chosen, axis=0, keepdims=True)


def estimate(flops):
    return pl.CostEstimate(flops=flops, bytes_accessed=10**6, transcendentals=0)


def shards(gx, gy, positions, node_moments, slot_of, block_list, tile_counts):
    count = positions.shape[1]
    tiles = count // LANES
    each = node_moments.shape[1] // LANES
    room = pl.cdiv(block_list.size + 2 * PAIRS + 1, LANES) * LANES
    vmem = pl.BlockSpec(memory_space=pltpu.VMEM)
    smem = pl.BlockSpec(memory_space=pltpu.SMEM)

    def swap(value, axis, size, bits):
        return lax.ppermute(value, axis, [(i, i ^ bits) for i in range(size)])

    def work(blocks):
        shapes = [
            pltpu.VMEM((blocks * FEATURES, LANES), jnp.float32),
            pltpu.VMEM((blocks * WEIGHTS, LANES), jnp.float32),
            pltpu.VMEM((PAIRS, LANES, 2 * LANES), jnp.float32),
            pltpu.VMEM((PAIRS, 4, LANES, LANES), jnp.bfloat16),
        ]
        rows = blocks * (FEATURES + WEIGHTS) + PAIRS * 4 * LANES + tiles * 2 * LANES
        limit = min(rows * 4 * LANES + 2**21, 60 * 1024 * 1024)
        return shapes, pltpu.CompilerParams(vmem_limit_bytes=limit)

    here = jnp.stack([lax.axis_index("gx"), lax.axis_index("gy")]).astype(jnp.int32)
    prepare = pl.pallas_call(
        functools.partial(prep_kernel, gx, gy, each),
        out_shape=(
            jax.ShapeDtypeStruct((3, tiles, LANES), jnp.float32),
            jax.ShapeDtypeStruct((3, LANES), jnp.float32),
            jax.ShapeDtypeStruct((tiles, LANES, LANES), jnp.bfloat16),
            jax.ShapeDtypeStruct((1, room), jnp.int32),
            jax.ShapeDtypeStruct((1, room), jnp.int32),
            jax.ShapeDtypeStruct((10 * each, LANES), jnp.float32),
        ),
        in_specs=[smem] + [pl.BlockSpec(memory_space=pltpu.HBM)] * 5,
        out_specs=(vmem,) * 6,
        scratch_shapes=[
            pltpu.VMEM((tiles * LANES, LANES), jnp.float32),
            pltpu.VMEM(block_list.shape, jnp.int32),
            pltpu.SMEM(tile_counts.shape, jnp.int32),
            pltpu.VMEM(positions.shape, jnp.float32),
            pltpu.VMEM(slot_of.shape, jnp.int32),
            pltpu.VMEM(node_moments.shape, jnp.float32),
            pltpu.SemaphoreType.DMA((5,)),
        ],
        compiler_params=pltpu.CompilerParams(vmem_limit_bytes=8 * 2**20),
        cost_estimate=estimate(10**10),
    )
    held = [
        pltpu.with_memory_space_constraint(value, pltpu.HBM)
        for value in (block_list, tile_counts, positions, slot_of, node_moments)
    ]
    tiled, origin, left, near_list, far_list, own = prepare(here, *held)
    near = [swap(node_moments, "gx", gx, b) for b in range(1, gx)]
    near = jnp.stack([own] + [value.reshape(10 * each, LANES) for value in near])
    near, origin = lax.optimization_barrier((near, origin))
    far = [swap(near, "gy", gy, b) for b in range(2, gy, 2)]
    near_twin = swap(near, "gy", gy, 1)
    near_work, near_params = work(2 * gx * each)
    near_pairs = pl.pallas_call(
        near_kernel,
        out_shape=jax.ShapeDtypeStruct((tiles + 1, LANES, LANES), jnp.float32),
        in_specs=[smem] + [vmem] * 4,
        out_specs=vmem,
        scratch_shapes=near_work,
        compiler_params=near_params,
        cost_estimate=estimate(10**10),
    )
    total = near_pairs(near_list, origin, left, near, near_twin)
    far = jnp.concatenate(far, axis=0)
    far, total = lax.optimization_barrier((far, total))
    far_twin = swap(far, "gy", gy, 1)
    far_work, far_params = work((gy - 2) * gx * each)
    return pl.pallas_call(
        far_kernel,
        out_shape=jax.ShapeDtypeStruct((3, count), jnp.float32),
        in_specs=[smem] + [vmem] * 7,
        out_specs=vmem,
        scratch_shapes=[
            pltpu.VMEM((tiles + 1, LANES, LANES), jnp.float32),
            pltpu.VMEM((pl.cdiv(tiles, 4) * LANES, LANES), jnp.float32),
        ]
        + far_work,
        compiler_params=far_params,
    )(far_list, tiled, origin, left, slot_of, far, far_twin, total)


def solution(mesh):
    placed = (
        P(None, ("gx", "gy")),
        P(None, ("gx", "gy")),
        P(("gx", "gy"), None),
        P(("gx", "gy"), None),
        P(("gx", "gy")),
    )

    def body(*args):
        return shards(mesh.shape["gx"], mesh.shape["gy"], *args)

    return jax.shard_map(
        body, mesh=mesh, in_specs=placed, out_specs=P(None, ("gx", "gy")), check_vma=False
    )
```

```python
import functools
import math

import jax
import jax.numpy as jnp
from jax import lax
from jax.experimental import pallas as pl
from jax.experimental.pallas import tpu as pltpu
from jax.sharding import PartitionSpec as P


LANES = 128
SUBS = 8
PAIRS = 8
FEATURES = 48
WEIGHTS = 40
BLOCK_ROOM = 2**16
split_a = 0.5
soft_sq = 0.25
root_pi = math.sqrt(math.pi)

ERFC_BIAS = 0.15
ERFC_POLY = (
    0.565651365,
    -0.0323440266,
    1.41906215,
    -1.34343713,
    0.938636763,
    -0.36025162,
    0.0669870813,
)

UNIT = split_a * split_a / math.log(2.0)
LEAD = ERFC_POLY[-1] * UNIT ** ((len(ERFC_POLY) - 1) / 2)
MONIC = tuple(coef * UNIT ** (i / 2) / LEAD for i, coef in enumerate(ERFC_POLY))[:-1]
BIAS = ERFC_BIAS * UNIT
SCALE = LEAD * UNIT
ADD_2 = 4.0 * split_a**3 / root_pi / 3.0 / SCALE
ADD_3 = 8.0 * split_a**5 / root_pi / 15.0 / (SCALE * UNIT)


def thirds(value):
    top = value.astype(jnp.bfloat16).astype(jnp.float32)
    rest = value - top
    mid = rest.astype(jnp.bfloat16).astype(jnp.float32)
    low = (rest - mid).astype(jnp.bfloat16).astype(jnp.float32)
    return top, mid, low


def quotient(value, by):
    if by & (by - 1) == 0:
        return lax.shift_right_logical(value, by.bit_length() - 1)
    return lax.div(value, by)


def hot_lanes(slots, count):
    lane = lax.bitwise_and(slots, LANES - 1)
    rows = lax.broadcasted_iota(jnp.int32, (LANES, count), 0)
    return jnp.where(rows == lane, 1.0, 0.0).astype(jnp.bfloat16)


def owners(slots, tiles, count):
    rows = lax.broadcasted_iota(jnp.int32, (tiles, count), 0)
    return rows == lax.shift_right_logical(slots, 7)


def prep_kernel(
    gx,
    gy,
    each,
    self_ref,
    lists_hbm,
    counts_hbm,
    pos_hbm,
    slot_hbm,
    nodes_hbm,
    tiled_ref,
    origin_ref,
    left_ref,
    near_list_ref,
    far_list_ref,
    own_ref,
    rows_ref,
    lists_ref,
    counts_ref,
    pos_ref,
    slot_ref,
    nodes_ref,
    sems,
):
    count = pos_ref.shape[1]
    tiles = count // LANES
    moves = (
        (pos_hbm, pos_ref),
        (slot_hbm, slot_ref),
        (lists_hbm, lists_ref),
        (counts_hbm, counts_ref),
        (nodes_hbm, nodes_ref),
    )
    copies = [
        pltpu.make_async_copy(source, target, sems.at[i])
        for i, (source, target) in enumerate(moves)
    ]
    for copy in copies:
        copy.start()
    for copy in copies:
        copy.wait()
    for j in range(each):
        own_ref[pl.ds(j, 10, stride=each), :] = nodes_ref[:, j * LANES : (j + 1) * LANES]
    slots = slot_ref[...]
    owner = owners(slots, tiles, count)
    hot = hot_lanes(slots, count)
    rows = []
    for c in range(3):
        value = pos_ref[c : c + 1, :]
        origin = jnp.sum(value, axis=1, keepdims=True) * (1.0 / count)
        origin_ref[c : c + 1, :] = jnp.broadcast_to(origin, (1, LANES))
        for part in thirds(value - origin):
            rows.append(jnp.where(owner, part, 0.0).astype(jnp.bfloat16))
    got = lax.dot_general(
        jnp.concatenate(rows, axis=0),
        hot,
        (((1,), (1,)), ((), ())),
        preferred_element_type=jnp.float32,
    )
    place = []
    for c in range(3):
        top, mid, low = (got[(3 * c + p) * tiles : (3 * c + p + 1) * tiles, :] for p in range(3))
        tiled_ref[c] = top + mid + low
        place.append(top + mid + low)
    x, y, z = place
    one = jnp.ones_like(x)
    zero = jnp.zeros_like(x)
    terms = [x, y, z, one, -UNIT * (x * x + y * y + (z * z + soft_sq)), x, y, z]
    terms += [x * x, y * y, z * z, x * y, x * z, y * z, one, zero]
    for i, term in enumerate(terms):
        for s, part in enumerate(thirds(term)):
            rows_ref[pl.ds(s * 16 + i, tiles, stride=FEATURES), :] = part
    blank = jnp.zeros((LANES - 2 * FEATURES, LANES), jnp.float32)
    for t in range(tiles):
        kind = [rows_ref[pl.ds(t * FEATURES + s * 16, 16), :] for s in range(3)]
        rows = jnp.concatenate([kind[s] for s in (0, 0, 0, 1, 1, 2)] + [blank], axis=0)
        left_ref[t] = rows.T.astype(jnp.bfloat16)

    block = lists_ref[...]
    length = block.shape[1]
    dev = quotient(block, each)
    far_x = quotient(dev, gy) ^ self_ref[0]
    far_y = (dev & (gy - 1)) ^ self_ref[1]
    core, far_z = far_y & 1, lax.shift_right_logical(far_y, 1)
    inside = block & (each - 1)
    near_at = (core * gx + far_x) * each + inside
    far_at = ((core * (gy // 2 - 1) + far_z - 1) * gx + far_x) * each + inside
    tile_of = lax.broadcasted_iota(jnp.int32, (tiles, length), 0)
    slot = lax.broadcasted_iota(jnp.int32, (tiles, length), 1)
    limit = jnp.zeros((tiles, length), jnp.int32)
    for t in range(tiles):
        limit = jnp.where(tile_of == t, counts_ref[t], limit)
    live = slot < limit
    before = lax.broadcasted_iota(jnp.int32, (length, length), 0)
    before = before < lax.broadcasted_iota(jnp.int32, (length, length), 1)
    above = lax.broadcasted_iota(jnp.int32, (tiles, tiles), 1)
    above = above < lax.broadcasted_iota(jnp.int32, (tiles, tiles), 0)
    for out_ref, member, at in (
        (near_list_ref, far_z == 0, near_at),
        (far_list_ref, far_z != 0, far_at),
    ):
        member = live & member
        hits = jnp.where(member, 1.0, 0.0)
        number = jnp.sum(hits, axis=1, keepdims=True)
        ahead = jnp.dot(
            hits.astype(jnp.bfloat16),
            jnp.where(before, 1.0, 0.0).astype(jnp.bfloat16),
            preferred_element_type=jnp.float32,
        )
        ahead += jnp.dot(
            jnp.where(above, 1.0, 0.0).astype(jnp.bfloat16),
            jnp.broadcast_to(number, (tiles, length)).astype(jnp.bfloat16),
            preferred_element_type=jnp.float32,
        )
        ahead = jnp.where(member, ahead, -1.0)
        room = out_ref.shape[1]
        entry = tile_of * BLOCK_ROOM + at - tiles * BLOCK_ROOM
        where = lax.broadcasted_iota(jnp.int32, (tiles, room), 1)
        total = jnp.zeros((tiles, room), jnp.int32)
        for k in range(length):
            mine = ahead[:, k : k + 1].astype(jnp.int32)
            total += jnp.where(where == mine, entry[:, k : k + 1], 0)
        total = jnp.sum(total, axis=0, keepdims=True) + tiles * BLOCK_ROOM
        last = lax.broadcasted_iota(jnp.int32, (1, room), 1) == room - 1
        total = jnp.where(last, jnp.sum(number).astype(jnp.int32), total)
        out_ref[...] = total


def node_features(origin_ref, nodes_ref, feats_ref, weights_ref, start):
    devices, rows, _ = nodes_ref.shape
    each = rows // 10
    group = max(1, SUBS // each)
    wide = group * each
    shape = (wide, LANES)
    centre = [jnp.broadcast_to(origin_ref[c : c + 1, :], shape) for c in range(3)]

    def some(i, carry):
        def row(r):
            parts = [
                nodes_ref[i * group + g, r * each : (r + 1) * each, :] for g in range(group)
            ]
            return parts[0] if group == 1 else jnp.concatenate(parts, axis=0)

        def put(ref, high, r, value):
            ref[pl.ds((start + i * wide) * high + r * wide, wide), :] = value

        mass = row(0)
        cx, cy, cz = (row(1 + c) - centre[c] for c in range(3))
        qxx, qyy, qzz, qxy, qxz, qyz = (row(4 + c) for c in range(6))
        vx = qxx * cx + qxy * cy + qxz * cz
        vy = qxy * cx + qyy * cy + qyz * cz
        vz = qxz * cx + qyz * cy + qzz * cz
        terms = [2.0 * UNIT * cx, 2.0 * UNIT * cy, 2.0 * UNIT * cz]
        terms += [-UNIT * (cx * cx + cy * cy + cz * cz)]
        one = (7.5 * UNIT**2) / mass
        two = one + one
        terms += [jnp.ones(shape, jnp.float32), -two * vx, -two * vy, -two * vz]
        terms += [one * qxx, one * qyy, one * qzz, two * qxy, two * qxz, two * qyz]
        terms += [one * (vx * cx + vy * cy + vz * cz)]
        for r, term in enumerate(terms):
            for s, part in enumerate(thirds(term)):
                put(feats_ref, FEATURES, s * 16 + r, part)
        for s in range(3):
            put(feats_ref, FEATURES, s * 16 + 15, jnp.zeros(shape, jnp.float32))
        half = (1.5 * UNIT) * (qxx + qyy + qzz)
        full = 3.0 * UNIT
        diag = [full * qxx + half, full * qyy + half, full * qzz + half]
        near = [full * vx + half * cx, full * vy + half * cy, full * vz + half * cz]
        zero = jnp.zeros(shape, jnp.float32)
        for c, value in enumerate((mass * cx, mass * cy, mass * cz)):
            for s, part in enumerate(thirds(value)):
                put(weights_ref, WEIGHTS, s * 3 + c, part)
        for s, part in enumerate(thirds(mass)):
            put(weights_ref, WEIGHTS, 9 + s, part)
        for r in range(12, 16):
            put(weights_ref, WEIGHTS, r, zero)
        for c, value in enumerate(near):
            for s, part in enumerate(thirds(value)):
                put(weights_ref, WEIGHTS, 16 + s * 3 + c, -part)
        for r in range(25, 28):
            put(weights_ref, WEIGHTS, r, zero)
        for c, value in enumerate(diag + [full * qxy, full * qxz, full * qyz]):
            top, mid, _ = thirds(value)
            put(weights_ref, WEIGHTS, 28 + c, top)
            put(weights_ref, WEIGHTS, 34 + c, mid)
        return carry

    lax.fori_loop(0, devices // group, some, 0)


def rows_of(ref, high, wide, block, first, number):
    base = quotient(block, wide) * (high * wide) + (block & (wide - 1))
    return ref[pl.ds(base + first * wide, number, stride=wide), :]


def distances(left, take, near_ref):
    rows = lax.broadcasted_iota(jnp.int32, (SUBS, LANES), 0)
    zero = jnp.zeros((SUBS, LANES), jnp.float32)
    first, second = [], []
    for s in range(3):
        one = take(s * 16, SUBS)
        two = take(s * 16 + SUBS, SUBS)
        first.append(jnp.concatenate([jnp.where(rows < 5, one, 0.0), zero], axis=0))
        second.append(
            jnp.concatenate(
                [jnp.where(rows >= 5, one, 0.0), two], axis=0
            )
        )
    blank = jnp.zeros((LANES - 96, 2 * LANES), jnp.float32)
    order = (0, 1, 2, 0, 1, 0)
    right = jnp.concatenate(
        [jnp.concatenate([first[s], second[s]], axis=1) for s in order] + [blank], axis=0
    ).astype(jnp.bfloat16)
    near_ref[...] = jnp.dot(left, right, preferred_element_type=jnp.float32)


def pair_terms(near_ref, terms_ref):
    step = 2 * SUBS
    for g in range(LANES // step):
        at = pl.ds(g * step, step)
        power = near_ref[at, 0:LANES]
        inner = near_ref[at, LANES : 2 * LANES]
        inv = lax.rsqrt(power * power)
        expo = jnp.exp2(power)
        arg = lax.rsqrt(BIAS - power)
        poly = arg + MONIC[-1]
        for coef in MONIC[-2::-1]:
            poly = poly * arg + coef
        first = poly * inv
        second = (first + ADD_2) * inv
        third = (second + ADD_3) * inv
        radial = (first + third * inner) * expo
        second = second * expo
        for i, value in enumerate((radial, second)):
            top = value.astype(jnp.bfloat16)
            low = (value - top.astype(jnp.float32)).astype(jnp.bfloat16)
            terms_ref[i, at, :] = top
            terms_ref[2 + i, at, :] = low


def add_forces(terms_ref, take, total_ref, tile):
    top = jnp.concatenate([take(0, 16), jnp.zeros((SUBS, LANES), jnp.float32)], axis=0)
    low = take(16, 24)
    right = jnp.concatenate([top, low], axis=1).astype(jnp.bfloat16)
    left = jnp.concatenate(
        [jnp.concatenate([terms_ref[i], terms_ref[i + 1]], axis=1) for i in (0, 2)], axis=0
    )
    got = lax.dot_general(
        left, right, (((1,), (1,)), ((), ())), preferred_element_type=jnp.float32
    )
    total_ref[tile, :, 0:24] += got[:LANES] + got[LANES:]


def all_pairs(list_ref, origin_ref, left_ref, mine_ref, twin_ref, total_ref, scratch):
    feats_ref, weights_ref, near_ref, terms_ref = scratch
    tiles = left_ref.shape[0]
    each = mine_ref.shape[1] // 10
    wide = max(1, SUBS // each) * each
    half = mine_ref.shape[0] * each
    node_features(origin_ref, mine_ref, feats_ref, weights_ref, 0)
    node_features(origin_ref, twin_ref, feats_ref, weights_ref, half)

    def ahead(u, n):
        entry = list_ref[0, n]
        tile, block = quotient(entry, BLOCK_ROOM), entry & (BLOCK_ROOM - 1)
        take = functools.partial(rows_of, feats_ref, FEATURES, wide, block)
        distances(left_ref[jnp.minimum(tile, tiles - 1)], take, near_ref.at[u])
        return tile, block

    def behind(u, pair):
        take = functools.partial(rows_of, weights_ref, WEIGHTS, wide, pair[1])
        add_forces(terms_ref.at[u], take, total_ref, pair[0])

    def step(i, carry):
        pairs, last = carry
        nexts = []
        behind(PAIRS - 1, last)
        for u in range(PAIRS):
            pair_terms(near_ref.at[u], terms_ref.at[u])
            nexts.append(ahead(u, (i + 1) * PAIRS + u))
            if u + 1 < PAIRS:
                behind(u, pairs[u])
        return tuple(nexts), pairs[-1]

    pairs = tuple(ahead(u, u) for u in range(PAIRS))
    none = (jnp.int32(tiles), jnp.int32(0))
    terms_ref[PAIRS - 1] = jnp.zeros(terms_ref.shape[1:], terms_ref.dtype)
    live = list_ref[0, list_ref.shape[1] - 1]
    steps = quotient(live + (PAIRS - 1), PAIRS)
    carry = lax.fori_loop(0, steps, step, (pairs, none))
    behind(PAIRS - 1, carry[-1])


def near_kernel(list_ref, origin_ref, left_ref, mine_ref, twin_ref, total_ref, *scratch):
    total_ref[...] = jnp.zeros_like(total_ref)
    all_pairs(list_ref, origin_ref, left_ref, mine_ref, twin_ref, total_ref, scratch)


def far_kernel(
    list_ref,
    tiled_ref,
    origin_ref,
    left_ref,
    slot_ref,
    mine_ref,
    twin_ref,
    start_ref,
    out_ref,
    total_ref,
    flat_ref,
    *scratch,
):
    count = slot_ref.shape[1]
    tiles = count // LANES
    total_ref[...] = start_ref[...]
    all_pairs(list_ref, origin_ref, left_ref, mine_ref, twin_ref, total_ref, scratch)
    room = LANES // 4
    for q in range(0, tiles, 4):
        four = total_ref[q]
        for j in range(1, min(4, tiles - q)):
            four += pltpu.roll(total_ref[q + j], room * j, 1)
        flat_ref[pl.ds(q * room, LANES), :] = four.T

    def column(r):
        return flat_ref[pl.ds(r, tiles, stride=room), :]

    x, y, z = tiled_ref[0], tiled_ref[1], tiled_ref[2]
    sums = column(9) + column(10) + column(11)
    mxx, myy, mzz, mxy, mxz, myz = (column(12 + c) + column(18 + c) for c in range(6))
    const = [column(c) + column(3 + c) + column(6 + c) for c in range(3)]
    forces = [
        SCALE * (const[0] - x * sums + (mxx * x + mxy * y + mxz * z)),
        SCALE * (const[1] - y * sums + (mxy * x + myy * y + myz * z)),
        SCALE * (const[2] - z * sums + (mxz * x + myz * y + mzz * z)),
    ]
    slots = slot_ref[...]
    owner = owners(slots, tiles, count)
    parts = [part.astype(jnp.bfloat16) for force in forces for part in thirds(force)]
    got = jnp.dot(
        jnp.concatenate(parts, axis=0),
        hot_lanes(slots, count),
        preferred_element_type=jnp.float32,
    )
    for c in range(3):
        top, mid, low = (got[(3 * c + p) * tiles : (3 * c + p + 1) * tiles, :] for p in range(3))
        chosen = jnp.where(owner, top + mid + low, 0.0)
        out_ref[c : c + 1, :] = jnp.sum(chosen, axis=0, keepdims=True)


def estimate(flops):
    return pl.CostEstimate(flops=flops, bytes_accessed=10**6, transcendentals=0)


def shards(gx, gy, positions, node_moments, slot_of, block_list, tile_counts):
    count = positions.shape[1]
    tiles = count // LANES
    each = node_moments.shape[1] // LANES
    room = pl.cdiv(block_list.size + 2 * PAIRS + 1, LANES) * LANES
    vmem = pl.BlockSpec(memory_space=pltpu.VMEM)
    smem = pl.BlockSpec(memory_space=pltpu.SMEM)

    def swap(value, axis, size, bits):
        return lax.ppermute(value, axis, [(i, i ^ bits) for i in range(size)])

    def work(blocks):
        shapes = [
            pltpu.VMEM((blocks * FEATURES, LANES), jnp.float32),
            pltpu.VMEM((blocks * WEIGHTS, LANES), jnp.float32),
            pltpu.VMEM((PAIRS, LANES, 2 * LANES), jnp.float32),
            pltpu.VMEM((PAIRS, 4, LANES, LANES), jnp.bfloat16),
        ]
        rows = blocks * (FEATURES + WEIGHTS) + PAIRS * 4 * LANES + tiles * 2 * LANES
        limit = min(rows * 4 * LANES + 2**21, 60 * 1024 * 1024)
        return shapes, pltpu.CompilerParams(vmem_limit_bytes=limit)

    here = jnp.stack([lax.axis_index("gx"), lax.axis_index("gy")]).astype(jnp.int32)
    prepare = pl.pallas_call(
        functools.partial(prep_kernel, gx, gy, each),
        out_shape=(
            jax.ShapeDtypeStruct((3, tiles, LANES), jnp.float32),
            jax.ShapeDtypeStruct((3, LANES), jnp.float32),
            jax.ShapeDtypeStruct((tiles, LANES, LANES), jnp.bfloat16),
            jax.ShapeDtypeStruct((1, room), jnp.int32),
            jax.ShapeDtypeStruct((1, room), jnp.int32),
            jax.ShapeDtypeStruct((10 * each, LANES), jnp.float32),
        ),
        in_specs=[smem] + [pl.BlockSpec(memory_space=pltpu.HBM)] * 5,
        out_specs=(vmem,) * 6,
        scratch_shapes=[
            pltpu.VMEM((tiles * FEATURES, LANES), jnp.float32),
            pltpu.VMEM(block_list.shape, jnp.int32),
            pltpu.SMEM(tile_counts.shape, jnp.int32),
            pltpu.VMEM(positions.shape, jnp.float32),
            pltpu.VMEM(slot_of.shape, jnp.int32),
            pltpu.VMEM(node_moments.shape, jnp.float32),
            pltpu.SemaphoreType.DMA((5,)),
        ],
        compiler_params=pltpu.CompilerParams(vmem_limit_bytes=8 * 2**20),
        cost_estimate=estimate(10**10),
    )
    held = [
        pltpu.with_memory_space_constraint(value, pltpu.HBM)
        for value in (block_list, tile_counts, positions, slot_of, node_moments)
    ]
    tiled, origin, left, near_list, far_list, own = prepare(here, *held)
    near = [swap(node_moments, "gx", gx, b) for b in range(1, gx)]
    near = jnp.stack([own] + [value.reshape(10 * each, LANES) for value in near])
    near, origin = lax.optimization_barrier((near, origin))
    far = [swap(near, "gy", gy, b) for b in range(2, gy, 2)]
    near_twin = swap(near, "gy", gy, 1)
    near_work, near_params = work(2 * gx * each)
    near_pairs = pl.pallas_call(
        near_kernel,
        out_shape=jax.ShapeDtypeStruct((tiles + 1, LANES, LANES), jnp.float32),
        in_specs=[smem] + [vmem] * 4,
        out_specs=vmem,
        scratch_shapes=near_work,
        compiler_params=near_params,
        cost_estimate=estimate(10**10),
    )
    total = near_pairs(near_list, origin, left, near, near_twin)
    far = jnp.concatenate(far, axis=0)
    far, total = lax.optimization_barrier((far, total))
    far_twin = swap(far, "gy", gy, 1)
    far_work, far_params = work((gy - 2) * gx * each)
    return pl.pallas_call(
        far_kernel,
        out_shape=jax.ShapeDtypeStruct((3, count), jnp.float32),
        in_specs=[smem] + [vmem] * 7,
        out_specs=vmem,
        scratch_shapes=[
            pltpu.VMEM((tiles + 1, LANES, LANES), jnp.float32),
            pltpu.VMEM((pl.cdiv(tiles, 4) * LANES, LANES), jnp.float32),
        ]
        + far_work,
        compiler_params=far_params,
    )(far_list, tiled, origin, left, slot_of, far, far_twin, total)


def solution(mesh):
    placed = (
        P(None, ("gx", "gy")),
        P(None, ("gx", "gy")),
        P(("gx", "gy"), None),
        P(("gx", "gy"), None),
        P(("gx", "gy")),
    )

    def body(*args):
        return shards(mesh.shape["gx"], mesh.shape["gy"], *args)

    return jax.shard_map(
        body, mesh=mesh, in_specs=placed, out_specs=P(None, ("gx", "gy")), check_vma=False
    )
```

```python
import functools
import math

import jax
import jax.numpy as jnp
from jax import lax
from jax.experimental import pallas as pl
from jax.experimental.pallas import tpu as pltpu
from jax.sharding import PartitionSpec as P


LANES = 128
SUBS = 8
PAIRS = 8
LAG = 2
FEATURES = 48
WEIGHTS = 40
BLOCK_ROOM = 2**16
split_a = 0.5
soft_sq = 0.25
root_pi = math.sqrt(math.pi)

ERFC_BIAS = 0.15
ERFC_POLY = (
    0.565651365,
    -0.0323440266,
    1.41906215,
    -1.34343713,
    0.938636763,
    -0.36025162,
    0.0669870813,
)

UNIT = split_a * split_a / math.log(2.0)
LEAD = ERFC_POLY[-1] * UNIT ** ((len(ERFC_POLY) - 1) / 2)
MONIC = tuple(coef * UNIT ** (i / 2) / LEAD for i, coef in enumerate(ERFC_POLY))[:-1]
BIAS = ERFC_BIAS * UNIT
SCALE = LEAD * UNIT
ADD_2 = 4.0 * split_a**3 / root_pi / 3.0 / SCALE
ADD_3 = 8.0 * split_a**5 / root_pi / 15.0 / (SCALE * UNIT)


def thirds(value):
    top = value.astype(jnp.bfloat16).astype(jnp.float32)
    rest = value - top
    mid = rest.astype(jnp.bfloat16).astype(jnp.float32)
    low = (rest - mid).astype(jnp.bfloat16).astype(jnp.float32)
    return top, mid, low


def quotient(value, by):
    if by & (by - 1) == 0:
        return lax.shift_right_logical(value, by.bit_length() - 1)
    return lax.div(value, by)


def hot_lanes(slots, count):
    lane = lax.bitwise_and(slots, LANES - 1)
    rows = lax.broadcasted_iota(jnp.int32, (LANES, count), 0)
    return jnp.where(rows == lane, 1.0, 0.0).astype(jnp.bfloat16)


def owners(slots, tiles, count):
    rows = lax.broadcasted_iota(jnp.int32, (tiles, count), 0)
    return rows == lax.shift_right_logical(slots, 7)


def prep_kernel(
    gx,
    gy,
    each,
    self_ref,
    lists_hbm,
    counts_hbm,
    pos_hbm,
    slot_hbm,
    nodes_hbm,
    tiled_ref,
    origin_ref,
    left_ref,
    near_list_ref,
    far_list_ref,
    own_ref,
    rows_ref,
    lists_ref,
    counts_ref,
    pos_ref,
    slot_ref,
    nodes_ref,
    sems,
):
    count = pos_ref.shape[1]
    tiles = count // LANES
    moves = (
        (pos_hbm, pos_ref),
        (slot_hbm, slot_ref),
        (lists_hbm, lists_ref),
        (counts_hbm, counts_ref),
        (nodes_hbm, nodes_ref),
    )
    copies = [
        pltpu.make_async_copy(source, target, sems.at[i])
        for i, (source, target) in enumerate(moves)
    ]
    for copy in copies:
        copy.start()
    for copy in copies:
        copy.wait()
    for j in range(each):
        own_ref[pl.ds(j, 10, stride=each), :] = nodes_ref[:, j * LANES : (j + 1) * LANES]
    slots = slot_ref[...]
    owner = owners(slots, tiles, count)
    hot = hot_lanes(slots, count)
    rows = []
    for c in range(3):
        value = pos_ref[c : c + 1, :]
        origin = jnp.sum(value, axis=1, keepdims=True) * (1.0 / count)
        origin_ref[c : c + 1, :] = jnp.broadcast_to(origin, (1, LANES))
        for part in thirds(value - origin):
            rows.append(jnp.where(owner, part, 0.0).astype(jnp.bfloat16))
    got = lax.dot_general(
        jnp.concatenate(rows, axis=0),
        hot,
        (((1,), (1,)), ((), ())),
        preferred_element_type=jnp.float32,
    )
    place = []
    for c in range(3):
        top, mid, low = (got[(3 * c + p) * tiles : (3 * c + p + 1) * tiles, :] for p in range(3))
        tiled_ref[c] = top + mid + low
        place.append(top + mid + low)
    x, y, z = place
    one = jnp.ones_like(x)
    zero = jnp.zeros_like(x)
    terms = [x, y, z, one, -UNIT * (x * x + y * y + (z * z + soft_sq)), x, y, z]
    terms += [x * x, y * y, z * z, x * y, x * z, y * z, one, zero]
    for i, term in enumerate(terms):
        for s, part in enumerate(thirds(term)):
            rows_ref[pl.ds(s * 16 + i, tiles, stride=FEATURES), :] = part
    blank = jnp.zeros((LANES - 2 * FEATURES, LANES), jnp.float32)
    for t in range(tiles):
        kind = [rows_ref[pl.ds(t * FEATURES + s * 16, 16), :] for s in range(3)]
        rows = jnp.concatenate([kind[s] for s in (0, 0, 0, 1, 1, 2)] + [blank], axis=0)
        left_ref[t] = rows.T.astype(jnp.bfloat16)

    block = lists_ref[...]
    length = block.shape[1]
    dev = quotient(block, each)
    far_x = quotient(dev, gy) ^ self_ref[0]
    far_y = (dev & (gy - 1)) ^ self_ref[1]
    core, far_z = far_y & 1, lax.shift_right_logical(far_y, 1)
    inside = block & (each - 1)
    near_at = (core * gx + far_x) * each + inside
    far_at = ((core * (gy // 2 - 1) + far_z - 1) * gx + far_x) * each + inside
    tile_of = lax.broadcasted_iota(jnp.int32, (tiles, length), 0)
    slot = lax.broadcasted_iota(jnp.int32, (tiles, length), 1)
    limit = jnp.zeros((tiles, length), jnp.int32)
    for t in range(tiles):
        limit = jnp.where(tile_of == t, counts_ref[t], limit)
    live = slot < limit
    before = lax.broadcasted_iota(jnp.int32, (length, length), 0)
    before = before < lax.broadcasted_iota(jnp.int32, (length, length), 1)
    above = lax.broadcasted_iota(jnp.int32, (tiles, tiles), 1)
    above = above < lax.broadcasted_iota(jnp.int32, (tiles, tiles), 0)
    for out_ref, member, at in (
        (near_list_ref, far_z == 0, near_at),
        (far_list_ref, far_z != 0, far_at),
    ):
        member = live & member
        hits = jnp.where(member, 1.0, 0.0)
        number = jnp.sum(hits, axis=1, keepdims=True)
        ahead = jnp.dot(
            hits.astype(jnp.bfloat16),
            jnp.where(before, 1.0, 0.0).astype(jnp.bfloat16),
            preferred_element_type=jnp.float32,
        )
        ahead += jnp.dot(
            jnp.where(above, 1.0, 0.0).astype(jnp.bfloat16),
            jnp.broadcast_to(number, (tiles, length)).astype(jnp.bfloat16),
            preferred_element_type=jnp.float32,
        )
        ahead = jnp.where(member, ahead, -1.0)
        room = out_ref.shape[1]
        entry = tile_of * BLOCK_ROOM + at - tiles * BLOCK_ROOM
        where = lax.broadcasted_iota(jnp.int32, (tiles, room), 1)
        total = jnp.zeros((tiles, room), jnp.int32)
        for k in range(length):
            mine = ahead[:, k : k + 1].astype(jnp.int32)
            total += jnp.where(where == mine, entry[:, k : k + 1], 0)
        total = jnp.sum(total, axis=0, keepdims=True) + tiles * BLOCK_ROOM
        last = lax.broadcasted_iota(jnp.int32, (1, room), 1) == room - 1
        total = jnp.where(last, jnp.sum(number).astype(jnp.int32), total)
        out_ref[...] = total


def node_features(origin_ref, nodes_ref, feats_ref, weights_ref, start):
    devices, rows, _ = nodes_ref.shape
    each = rows // 10
    group = max(1, SUBS // each)
    wide = group * each
    shape = (wide, LANES)
    centre = [jnp.broadcast_to(origin_ref[c : c + 1, :], shape) for c in range(3)]

    def some(i, carry):
        def row(r):
            parts = [
                nodes_ref[i * group + g, r * each : (r + 1) * each, :] for g in range(group)
            ]
            return parts[0] if group == 1 else jnp.concatenate(parts, axis=0)

        def put(ref, high, r, value):
            ref[pl.ds((start + i * wide) * high + r * wide, wide), :] = value

        mass = row(0)
        cx, cy, cz = (row(1 + c) - centre[c] for c in range(3))
        qxx, qyy, qzz, qxy, qxz, qyz = (row(4 + c) for c in range(6))
        vx = qxx * cx + qxy * cy + qxz * cz
        vy = qxy * cx + qyy * cy + qyz * cz
        vz = qxz * cx + qyz * cy + qzz * cz
        terms = [2.0 * UNIT * cx, 2.0 * UNIT * cy, 2.0 * UNIT * cz]
        terms += [-UNIT * (cx * cx + cy * cy + cz * cz)]
        one = (7.5 * UNIT**2) / mass
        two = one + one
        terms += [jnp.ones(shape, jnp.float32), -two * vx, -two * vy, -two * vz]
        terms += [one * qxx, one * qyy, one * qzz, two * qxy, two * qxz, two * qyz]
        terms += [one * (vx * cx + vy * cy + vz * cz)]
        for r, term in enumerate(terms):
            for s, part in enumerate(thirds(term)):
                put(feats_ref, FEATURES, s * 16 + r, part)
        for s in range(3):
            put(feats_ref, FEATURES, s * 16 + 15, jnp.zeros(shape, jnp.float32))
        half = (1.5 * UNIT) * (qxx + qyy + qzz)
        full = 3.0 * UNIT
        diag = [full * qxx + half, full * qyy + half, full * qzz + half]
        near = [full * vx + half * cx, full * vy + half * cy, full * vz + half * cz]
        zero = jnp.zeros(shape, jnp.float32)
        for c, value in enumerate((mass * cx, mass * cy, mass * cz)):
            for s, part in enumerate(thirds(value)):
                put(weights_ref, WEIGHTS, s * 3 + c, part)
        for s, part in enumerate(thirds(mass)):
            put(weights_ref, WEIGHTS, 9 + s, part)
        for r in range(12, 16):
            put(weights_ref, WEIGHTS, r, zero)
        for c, value in enumerate(near):
            for s, part in enumerate(thirds(value)):
                put(weights_ref, WEIGHTS, 16 + s * 3 + c, -part)
        for r in range(25, 28):
            put(weights_ref, WEIGHTS, r, zero)
        for c, value in enumerate(diag + [full * qxy, full * qxz, full * qyz]):
            top, mid, _ = thirds(value)
            put(weights_ref, WEIGHTS, 28 + c, top)
            put(weights_ref, WEIGHTS, 34 + c, mid)
        return carry

    lax.fori_loop(0, devices // group, some, 0)


def rows_of(ref, high, wide, block, first, number):
    base = quotient(block, wide) * (high * wide) + (block & (wide - 1))
    return ref[pl.ds(base + first * wide, number, stride=wide), :]


def distances(left, take, near_ref):
    rows = lax.broadcasted_iota(jnp.int32, (SUBS, LANES), 0)
    zero = jnp.zeros((SUBS, LANES), jnp.float32)
    first, second = [], []
    for s in range(3):
        one = take(s * 16, SUBS)
        two = take(s * 16 + SUBS, SUBS)
        first.append(jnp.concatenate([jnp.where(rows < 5, one, 0.0), zero], axis=0))
        second.append(
            jnp.concatenate(
                [jnp.where(rows >= 5, one, 0.0), two], axis=0
            )
        )
    blank = jnp.zeros((LANES - 96, 2 * LANES), jnp.float32)
    order = (0, 1, 2, 0, 1, 0)
    right = jnp.concatenate(
        [jnp.concatenate([first[s], second[s]], axis=1) for s in order] + [blank], axis=0
    ).astype(jnp.bfloat16)
    near_ref[...] = jnp.dot(left, right, preferred_element_type=jnp.float32)


def pair_terms(near_ref, terms_ref):
    step = 2 * SUBS
    for g in range(LANES // step):
        at = pl.ds(g * step, step)
        power = near_ref[at, 0:LANES]
        inner = near_ref[at, LANES : 2 * LANES]
        inv = lax.rsqrt(power * power)
        expo = jnp.exp2(power)
        arg = lax.rsqrt(BIAS - power)
        poly = arg + MONIC[-1]
        for coef in MONIC[-2::-1]:
            poly = poly * arg + coef
        first = poly * inv
        second = (first + ADD_2) * inv
        third = (second + ADD_3) * inv
        radial = (first + third * inner) * expo
        second = second * expo
        for i, value in enumerate((radial, second)):
            top = value.astype(jnp.bfloat16)
            low = (value - top.astype(jnp.float32)).astype(jnp.bfloat16)
            terms_ref[i, at, :] = top
            terms_ref[2 + i, at, :] = low


def add_forces(terms_ref, take, total_ref, tile):
    top = jnp.concatenate([take(0, 16), jnp.zeros((SUBS, LANES), jnp.float32)], axis=0)
    low = take(16, 24)
    right = jnp.concatenate([top, low], axis=1).astype(jnp.bfloat16)
    left = jnp.concatenate(
        [jnp.concatenate([terms_ref[i], terms_ref[i + 1]], axis=1) for i in (0, 2)], axis=0
    )
    got = lax.dot_general(
        left, right, (((1,), (1,)), ((), ())), preferred_element_type=jnp.float32
    )
    total_ref[tile, :, 0:24] += got[:LANES] + got[LANES:]


def all_pairs(list_ref, origin_ref, left_ref, mine_ref, twin_ref, total_ref, scratch):
    feats_ref, weights_ref, near_ref, terms_ref = scratch
    tiles = left_ref.shape[0]
    each = mine_ref.shape[1] // 10
    wide = max(1, SUBS // each) * each
    half = mine_ref.shape[0] * each
    node_features(origin_ref, mine_ref, feats_ref, weights_ref, 0)
    node_features(origin_ref, twin_ref, feats_ref, weights_ref, half)

    def ahead(u, n):
        entry = list_ref[0, n]
        tile, block = quotient(entry, BLOCK_ROOM), entry & (BLOCK_ROOM - 1)
        take = functools.partial(rows_of, feats_ref, FEATURES, wide, block)
        distances(left_ref[jnp.minimum(tile, tiles - 1)], take, near_ref.at[u])
        return tile, block

    def behind(u, pair):
        take = functools.partial(rows_of, weights_ref, WEIGHTS, wide, pair[1])
        add_forces(terms_ref.at[u], take, total_ref, pair[0])

    def step(i, carry):
        pairs, lasts = carry
        nexts = []
        for u in range(LAG):
            behind(PAIRS - LAG + u, lasts[u])
        for u in range(PAIRS):
            pair_terms(near_ref.at[u], terms_ref.at[u])
            nexts.append(ahead(u, (i + 1) * PAIRS + u))
            if u + LAG < PAIRS:
                behind(u, pairs[u])
        return tuple(nexts), pairs[-LAG:]

    pairs = tuple(ahead(u, u) for u in range(PAIRS))
    none = (jnp.int32(tiles), jnp.int32(0))
    for u in range(PAIRS - LAG, PAIRS):
        terms_ref[u] = jnp.zeros(terms_ref.shape[1:], terms_ref.dtype)
    live = list_ref[0, list_ref.shape[1] - 1]
    steps = quotient(live + (PAIRS - 1), PAIRS)
    carry = lax.fori_loop(0, steps, step, (pairs, (none,) * LAG))
    for u in range(LAG):
        behind(PAIRS - LAG + u, carry[-1][u])


def near_kernel(list_ref, origin_ref, left_ref, mine_ref, twin_ref, total_ref, *scratch):
    total_ref[...] = jnp.zeros_like(total_ref)
    all_pairs(list_ref, origin_ref, left_ref, mine_ref, twin_ref, total_ref, scratch)


def far_kernel(
    list_ref,
    tiled_ref,
    origin_ref,
    left_ref,
    slot_ref,
    mine_ref,
    twin_ref,
    start_ref,
    out_ref,
    total_ref,
    flat_ref,
    *scratch,
):
    count = slot_ref.shape[1]
    tiles = count // LANES
    total_ref[...] = start_ref[...]
    all_pairs(list_ref, origin_ref, left_ref, mine_ref, twin_ref, total_ref, scratch)
    room = LANES // 4
    for q in range(0, tiles, 4):
        four = total_ref[q]
        for j in range(1, min(4, tiles - q)):
            four += pltpu.roll(total_ref[q + j], room * j, 1)
        flat_ref[pl.ds(q * room, LANES), :] = four.T

    def column(r):
        return flat_ref[pl.ds(r, tiles, stride=room), :]

    x, y, z = tiled_ref[0], tiled_ref[1], tiled_ref[2]
    sums = column(9) + column(10) + column(11)
    mxx, myy, mzz, mxy, mxz, myz = (column(12 + c) + column(18 + c) for c in range(6))
    const = [column(c) + column(3 + c) + column(6 + c) for c in range(3)]
    forces = [
        SCALE * (const[0] - x * sums + (mxx * x + mxy * y + mxz * z)),
        SCALE * (const[1] - y * sums + (mxy * x + myy * y + myz * z)),
        SCALE * (const[2] - z * sums + (mxz * x + myz * y + mzz * z)),
    ]
    slots = slot_ref[...]
    owner = owners(slots, tiles, count)
    parts = [part.astype(jnp.bfloat16) for force in forces for part in thirds(force)]
    got = jnp.dot(
        jnp.concatenate(parts, axis=0),
        hot_lanes(slots, count),
        preferred_element_type=jnp.float32,
    )
    for c in range(3):
        top, mid, low = (got[(3 * c + p) * tiles : (3 * c + p + 1) * tiles, :] for p in range(3))
        chosen = jnp.where(owner, top + mid + low, 0.0)
        out_ref[c : c + 1, :] = jnp.sum(chosen, axis=0, keepdims=True)


def estimate(flops):
    return pl.CostEstimate(flops=flops, bytes_accessed=10**6, transcendentals=0)


def shards(gx, gy, positions, node_moments, slot_of, block_list, tile_counts):
    count = positions.shape[1]
    tiles = count // LANES
    each = node_moments.shape[1] // LANES
    room = pl.cdiv(block_list.size + 2 * PAIRS + 1, LANES) * LANES
    vmem = pl.BlockSpec(memory_space=pltpu.VMEM)
    smem = pl.BlockSpec(memory_space=pltpu.SMEM)

    def swap(value, axis, size, bits):
        return lax.ppermute(value, axis, [(i, i ^ bits) for i in range(size)])

    def work(blocks):
        shapes = [
            pltpu.VMEM((blocks * FEATURES, LANES), jnp.float32),
            pltpu.VMEM((blocks * WEIGHTS, LANES), jnp.float32),
            pltpu.VMEM((PAIRS, LANES, 2 * LANES), jnp.float32),
            pltpu.VMEM((PAIRS, 4, LANES, LANES), jnp.bfloat16),
        ]
        rows = blocks * (FEATURES + WEIGHTS) + PAIRS * 4 * LANES + tiles * 2 * LANES
        limit = min(rows * 4 * LANES + 2**21, 60 * 1024 * 1024)
        return shapes, pltpu.CompilerParams(vmem_limit_bytes=limit)

    here = jnp.stack([lax.axis_index("gx"), lax.axis_index("gy")]).astype(jnp.int32)
    prepare = pl.pallas_call(
        functools.partial(prep_kernel, gx, gy, each),
        out_shape=(
            jax.ShapeDtypeStruct((3, tiles, LANES), jnp.float32),
            jax.ShapeDtypeStruct((3, LANES), jnp.float32),
            jax.ShapeDtypeStruct((tiles, LANES, LANES), jnp.bfloat16),
            jax.ShapeDtypeStruct((1, room), jnp.int32),
            jax.ShapeDtypeStruct((1, room), jnp.int32),
            jax.ShapeDtypeStruct((10 * each, LANES), jnp.float32),
        ),
        in_specs=[smem] + [pl.BlockSpec(memory_space=pltpu.HBM)] * 5,
        out_specs=(vmem,) * 6,
        scratch_shapes=[
            pltpu.VMEM((tiles * FEATURES, LANES), jnp.float32),
            pltpu.VMEM(block_list.shape, jnp.int32),
            pltpu.SMEM(tile_counts.shape, jnp.int32),
            pltpu.VMEM(positions.shape, jnp.float32),
            pltpu.VMEM(slot_of.shape, jnp.int32),
            pltpu.VMEM(node_moments.shape, jnp.float32),
            pltpu.SemaphoreType.DMA((5,)),
        ],
        compiler_params=pltpu.CompilerParams(vmem_limit_bytes=8 * 2**20),
        cost_estimate=estimate(10**10),
    )
    held = [
        pltpu.with_memory_space_constraint(value, pltpu.HBM)
        for value in (block_list, tile_counts, positions, slot_of, node_moments)
    ]
    tiled, origin, left, near_list, far_list, own = prepare(here, *held)
    near = [swap(node_moments, "gx", gx, b) for b in range(1, gx)]
    near = jnp.stack([own] + [value.reshape(10 * each, LANES) for value in near])
    near, origin = lax.optimization_barrier((near, origin))
    far = [swap(near, "gy", gy, b) for b in range(2, gy, 2)]
    near_twin = swap(near, "gy", gy, 1)
    near_work, near_params = work(2 * gx * each)
    near_pairs = pl.pallas_call(
        near_kernel,
        out_shape=jax.ShapeDtypeStruct((tiles + 1, LANES, LANES), jnp.float32),
        in_specs=[smem] + [vmem] * 4,
        out_specs=vmem,
        scratch_shapes=near_work,
        compiler_params=near_params,
        cost_estimate=estimate(10**10),
    )
    total = near_pairs(near_list, origin, left, near, near_twin)
    far = jnp.concatenate(far, axis=0)
    far, total = lax.optimization_barrier((far, total))
    far_twin = swap(far, "gy", gy, 1)
    far_work, far_params = work((gy - 2) * gx * each)
    return pl.pallas_call(
        far_kernel,
        out_shape=jax.ShapeDtypeStruct((3, count), jnp.float32),
        in_specs=[smem] + [vmem] * 7,
        out_specs=vmem,
        scratch_shapes=[
            pltpu.VMEM((tiles + 1, LANES, LANES), jnp.float32),
            pltpu.VMEM((pl.cdiv(tiles, 4) * LANES, LANES), jnp.float32),
        ]
        + far_work,
        compiler_params=far_params,
    )(far_list, tiled, origin, left, slot_of, far, far_twin, total)


def solution(mesh):
    placed = (
        P(None, ("gx", "gy")),
        P(None, ("gx", "gy")),
        P(("gx", "gy"), None),
        P(("gx", "gy"), None),
        P(("gx", "gy")),
    )

    def body(*args):
        return shards(mesh.shape["gx"], mesh.shape["gy"], *args)

    return jax.shard_map(
        body, mesh=mesh, in_specs=placed, out_specs=P(None, ("gx", "gy")), check_vma=False
    )
```

```python
import functools
import math

import jax
import jax.numpy as jnp
from jax import lax
from jax.experimental import pallas as pl
from jax.experimental.pallas import tpu as pltpu
from jax.sharding import PartitionSpec as P


LANES = 128
SUBS = 8
PAIRS = 6
LAG = 2
FEATURES = 48
WEIGHTS = 40
BLOCK_ROOM = 2**16
split_a = 0.5
soft_sq = 0.25
root_pi = math.sqrt(math.pi)

ERFC_BIAS = 0.15
ERFC_POLY = (
    0.565651365,
    -0.0323440266,
    1.41906215,
    -1.34343713,
    0.938636763,
    -0.36025162,
    0.0669870813,
)

UNIT = split_a * split_a / math.log(2.0)
LEAD = ERFC_POLY[-1] * UNIT ** ((len(ERFC_POLY) - 1) / 2)
MONIC = tuple(coef * UNIT ** (i / 2) / LEAD for i, coef in enumerate(ERFC_POLY))[:-1]
BIAS = ERFC_BIAS * UNIT
SCALE = LEAD * UNIT
ADD_2 = 4.0 * split_a**3 / root_pi / 3.0 / SCALE
ADD_3 = 8.0 * split_a**5 / root_pi / 15.0 / (SCALE * UNIT)


def thirds(value):
    top = value.astype(jnp.bfloat16).astype(jnp.float32)
    rest = value - top
    mid = rest.astype(jnp.bfloat16).astype(jnp.float32)
    low = (rest - mid).astype(jnp.bfloat16).astype(jnp.float32)
    return top, mid, low


def quotient(value, by):
    if by & (by - 1) == 0:
        return lax.shift_right_logical(value, by.bit_length() - 1)
    return lax.div(value, by)


def hot_lanes(slots, count):
    lane = lax.bitwise_and(slots, LANES - 1)
    rows = lax.broadcasted_iota(jnp.int32, (LANES, count), 0)
    return jnp.where(rows == lane, 1.0, 0.0).astype(jnp.bfloat16)


def owners(slots, tiles, count):
    rows = lax.broadcasted_iota(jnp.int32, (tiles, count), 0)
    return rows == lax.shift_right_logical(slots, 7)


def prep_kernel(
    gx,
    gy,
    each,
    self_ref,
    lists_hbm,
    counts_hbm,
    pos_hbm,
    slot_hbm,
    nodes_hbm,
    tiled_ref,
    origin_ref,
    left_ref,
    near_list_ref,
    far_list_ref,
    own_ref,
    hot_ref,
    rows_ref,
    lists_ref,
    counts_ref,
    pos_ref,
    slot_ref,
    nodes_ref,
    sems,
):
    count = pos_ref.shape[1]
    tiles = count // LANES
    moves = (
        (pos_hbm, pos_ref),
        (slot_hbm, slot_ref),
        (lists_hbm, lists_ref),
        (counts_hbm, counts_ref),
        (nodes_hbm, nodes_ref),
    )
    copies = [
        pltpu.make_async_copy(source, target, sems.at[i])
        for i, (source, target) in enumerate(moves)
    ]
    for copy in copies:
        copy.start()
    for copy in copies:
        copy.wait()
    for j in range(each):
        own_ref[pl.ds(j, 10, stride=each), :] = nodes_ref[:, j * LANES : (j + 1) * LANES]
    slots = slot_ref[...]
    owner = owners(slots, tiles, count)
    hot = hot_lanes(slots, count)
    hot_ref[...] = hot
    rows = []
    for c in range(3):
        value = pos_ref[c : c + 1, :]
        origin = jnp.sum(value, axis=1, keepdims=True) * (1.0 / count)
        origin_ref[c : c + 1, :] = jnp.broadcast_to(origin, (1, LANES))
        for part in thirds(value - origin):
            rows.append(jnp.where(owner, part, 0.0).astype(jnp.bfloat16))
    got = lax.dot_general(
        jnp.concatenate(rows, axis=0),
        hot,
        (((1,), (1,)), ((), ())),
        preferred_element_type=jnp.float32,
    )
    place = []
    for c in range(3):
        top, mid, low = (got[(3 * c + p) * tiles : (3 * c + p + 1) * tiles, :] for p in range(3))
        tiled_ref[c] = top + mid + low
        place.append(top + mid + low)
    x, y, z = place
    one = jnp.ones_like(x)
    zero = jnp.zeros_like(x)
    terms = [x, y, z, one, -UNIT * (x * x + y * y + (z * z + soft_sq)), x, y, z]
    terms += [x * x, y * y, z * z, x * y, x * z, y * z, one, zero]
    for i, term in enumerate(terms):
        for s, part in enumerate(thirds(term)):
            rows_ref[pl.ds(s * 16 + i, tiles, stride=FEATURES), :] = part
    blank = jnp.zeros((LANES - 2 * FEATURES, LANES), jnp.float32)
    for t in range(tiles):
        kind = [rows_ref[pl.ds(t * FEATURES + s * 16, 16), :] for s in range(3)]
        rows = jnp.concatenate([kind[s] for s in (0, 0, 0, 1, 1, 2)] + [blank], axis=0)
        left_ref[t] = rows.T.astype(jnp.bfloat16)

    block = lists_ref[...]
    length = block.shape[1]
    dev = quotient(block, each)
    far_x = quotient(dev, gy) ^ self_ref[0]
    far_y = (dev & (gy - 1)) ^ self_ref[1]
    core, far_z = far_y & 1, lax.shift_right_logical(far_y, 1)
    inside = block & (each - 1)
    near_at = (core * gx + far_x) * each + inside
    far_at = ((core * (gy // 2 - 1) + far_z - 1) * gx + far_x) * each + inside
    tile_of = lax.broadcasted_iota(jnp.int32, (tiles, length), 0)
    slot = lax.broadcasted_iota(jnp.int32, (tiles, length), 1)
    limit = jnp.zeros((tiles, length), jnp.int32)
    for t in range(tiles):
        limit = jnp.where(tile_of == t, counts_ref[t], limit)
    live = slot < limit
    before = lax.broadcasted_iota(jnp.int32, (length, length), 0)
    before = before < lax.broadcasted_iota(jnp.int32, (length, length), 1)
    above = lax.broadcasted_iota(jnp.int32, (tiles, tiles), 1)
    above = above < lax.broadcasted_iota(jnp.int32, (tiles, tiles), 0)
    for out_ref, member, at in (
        (near_list_ref, far_z == 0, near_at),
        (far_list_ref, far_z != 0, far_at),
    ):
        member = live & member
        hits = jnp.where(member, 1.0, 0.0)
        number = jnp.sum(hits, axis=1, keepdims=True)
        ahead = jnp.dot(
            hits.astype(jnp.bfloat16),
            jnp.where(before, 1.0, 0.0).astype(jnp.bfloat16),
            preferred_element_type=jnp.float32,
        )
        ahead += jnp.dot(
            jnp.where(above, 1.0, 0.0).astype(jnp.bfloat16),
            jnp.broadcast_to(number, (tiles, length)).astype(jnp.bfloat16),
            preferred_element_type=jnp.float32,
        )
        ahead = jnp.where(member, ahead, -1.0)
        room = out_ref.shape[1]
        entry = tile_of * BLOCK_ROOM + at - tiles * BLOCK_ROOM
        where = lax.broadcasted_iota(jnp.int32, (tiles, room), 1)
        total = jnp.zeros((tiles, room), jnp.int32)
        for k in range(length):
            mine = ahead[:, k : k + 1].astype(jnp.int32)
            total += jnp.where(where == mine, entry[:, k : k + 1], 0)
        total = jnp.sum(total, axis=0, keepdims=True) + tiles * BLOCK_ROOM
        last = lax.broadcasted_iota(jnp.int32, (1, room), 1) == room - 1
        total = jnp.where(last, jnp.sum(number).astype(jnp.int32), total)
        out_ref[...] = total


def node_features(origin_ref, nodes_ref, feats_ref, weights_ref, start):
    devices, rows, _ = nodes_ref.shape
    each = rows // 10
    group = max(1, SUBS // each)
    wide = group * each
    shape = (wide, LANES)
    centre = [jnp.broadcast_to(origin_ref[c : c + 1, :], shape) for c in range(3)]

    def some(i, carry):
        def row(r):
            parts = [
                nodes_ref[i * group + g, r * each : (r + 1) * each, :] for g in range(group)
            ]
            return parts[0] if group == 1 else jnp.concatenate(parts, axis=0)

        def put(ref, high, r, value):
            ref[pl.ds((start + i * wide) * high + r * wide, wide), :] = value

        mass = row(0)
        cx, cy, cz = (row(1 + c) - centre[c] for c in range(3))
        qxx, qyy, qzz, qxy, qxz, qyz = (row(4 + c) for c in range(6))
        vx = qxx * cx + qxy * cy + qxz * cz
        vy = qxy * cx + qyy * cy + qyz * cz
        vz = qxz * cx + qyz * cy + qzz * cz
        terms = [2.0 * UNIT * cx, 2.0 * UNIT * cy, 2.0 * UNIT * cz]
        terms += [-UNIT * (cx * cx + cy * cy + cz * cz)]
        one = (7.5 * UNIT**2) / mass
        two = one + one
        terms += [jnp.ones(shape, jnp.float32), -two * vx, -two * vy, -two * vz]
        terms += [one * qxx, one * qyy, one * qzz, two * qxy, two * qxz, two * qyz]
        terms += [one * (vx * cx + vy * cy + vz * cz)]
        for r, term in enumerate(terms):
            for s, part in enumerate(thirds(term)):
                put(feats_ref, FEATURES, s * 16 + r, part)
        for s in range(3):
            put(feats_ref, FEATURES, s * 16 + 15, jnp.zeros(shape, jnp.float32))
        half = (1.5 * UNIT) * (qxx + qyy + qzz)
        full = 3.0 * UNIT
        diag = [full * qxx + half, full * qyy + half, full * qzz + half]
        near = [full * vx + half * cx, full * vy + half * cy, full * vz + half * cz]
        zero = jnp.zeros(shape, jnp.float32)
        for c, value in enumerate((mass * cx, mass * cy, mass * cz)):
            for s, part in enumerate(thirds(value)):
                put(weights_ref, WEIGHTS, s * 3 + c, part)
        for s, part in enumerate(thirds(mass)):
            put(weights_ref, WEIGHTS, 9 + s, part)
        for r in range(12, 16):
            put(weights_ref, WEIGHTS, r, zero)
        for c, value in enumerate(near):
            for s, part in enumerate(thirds(value)):
                put(weights_ref, WEIGHTS, 16 + s * 3 + c, -part)
        for r in range(25, 28):
            put(weights_ref, WEIGHTS, r, zero)
        for c, value in enumerate(diag + [full * qxy, full * qxz, full * qyz]):
            top, mid, _ = thirds(value)
            put(weights_ref, WEIGHTS, 28 + c, top)
            put(weights_ref, WEIGHTS, 34 + c, mid)
        return carry

    lax.fori_loop(0, devices // group, some, 0)


def rows_of(ref, high, wide, block, first, number):
    base = quotient(block, wide) * (high * wide) + (block & (wide - 1))
    return ref[pl.ds(base + first * wide, number, stride=wide), :]


def distances(left, take, near_ref):
    rows = lax.broadcasted_iota(jnp.int32, (SUBS, LANES), 0)
    zero = jnp.zeros((SUBS, LANES), jnp.float32)
    first, second = [], []
    for s in range(3):
        one = take(s * 16, SUBS)
        two = take(s * 16 + SUBS, SUBS)
        first.append(jnp.concatenate([jnp.where(rows < 5, one, 0.0), zero], axis=0))
        second.append(
            jnp.concatenate(
                [jnp.where(rows >= 5, one, 0.0), two], axis=0
            )
        )
    blank = jnp.zeros((LANES - 96, 2 * LANES), jnp.float32)
    order = (0, 1, 2, 0, 1, 0)
    right = jnp.concatenate(
        [jnp.concatenate([first[s], second[s]], axis=1) for s in order] + [blank], axis=0
    ).astype(jnp.bfloat16)
    near_ref[...] = jnp.dot(left, right, preferred_element_type=jnp.float32)


def pair_terms(near_ref, terms_ref):
    step = 2 * SUBS
    for g in range(LANES // step):
        at = pl.ds(g * step, step)
        power = near_ref[at, 0:LANES]
        inner = near_ref[at, LANES : 2 * LANES]
        inv = lax.rsqrt(power * power)
        expo = jnp.exp2(power)
        arg = lax.rsqrt(BIAS - power)
        poly = arg + MONIC[-1]
        for coef in MONIC[-2::-1]:
            poly = poly * arg + coef
        first = poly * inv
        second = (first + ADD_2) * inv
        third = (second + ADD_3) * inv
        radial = (first + third * inner) * expo
        second = second * expo
        for i, value in enumerate((radial, second)):
            top = value.astype(jnp.bfloat16)
            low = (value - top.astype(jnp.float32)).astype(jnp.bfloat16)
            terms_ref[i, at, :] = top
            terms_ref[2 + i, at, :] = low


def add_forces(terms_ref, take, total_ref, tile):
    top = jnp.concatenate([take(0, 16), jnp.zeros((SUBS, LANES), jnp.float32)], axis=0)
    low = take(16, 24)
    right = jnp.concatenate([top, low], axis=1).astype(jnp.bfloat16)
    left = jnp.concatenate(
        [jnp.concatenate([terms_ref[i], terms_ref[i + 1]], axis=1) for i in (0, 2)], axis=0
    )
    got = lax.dot_general(
        left, right, (((1,), (1,)), ((), ())), preferred_element_type=jnp.float32
    )
    total_ref[tile, :, 0:24] += got[:LANES] + got[LANES:]


def all_pairs(list_ref, origin_ref, left_ref, mine_ref, twin_ref, total_ref, scratch):
    feats_ref, weights_ref, near_ref, terms_ref = scratch
    tiles = left_ref.shape[0]
    each = mine_ref.shape[1] // 10
    wide = max(1, SUBS // each) * each
    half = mine_ref.shape[0] * each
    node_features(origin_ref, mine_ref, feats_ref, weights_ref, 0)
    node_features(origin_ref, twin_ref, feats_ref, weights_ref, half)

    def ahead(u, n):
        entry = list_ref[0, n]
        tile, block = quotient(entry, BLOCK_ROOM), entry & (BLOCK_ROOM - 1)
        take = functools.partial(rows_of, feats_ref, FEATURES, wide, block)
        distances(left_ref[jnp.minimum(tile, tiles - 1)], take, near_ref.at[u])
        return tile, block

    def behind(u, pair):
        take = functools.partial(rows_of, weights_ref, WEIGHTS, wide, pair[1])
        add_forces(terms_ref.at[u], take, total_ref, pair[0])

    def step(i, carry):
        pairs, lasts = carry
        nexts = []
        for u in range(LAG):
            behind(PAIRS - LAG + u, lasts[u])
        for u in range(PAIRS):
            pair_terms(near_ref.at[u], terms_ref.at[u])
            nexts.append(ahead(u, (i + 1) * PAIRS + u))
            if u + LAG < PAIRS:
                behind(u, pairs[u])
        return tuple(nexts), pairs[-LAG:]

    pairs = tuple(ahead(u, u) for u in range(PAIRS))
    none = (jnp.int32(tiles), jnp.int32(0))
    for u in range(PAIRS - LAG, PAIRS):
        terms_ref[u] = jnp.zeros(terms_ref.shape[1:], terms_ref.dtype)
    live = list_ref[0, list_ref.shape[1] - 1]
    steps = quotient(live + (PAIRS - 1), PAIRS)
    carry = lax.fori_loop(0, steps, step, (pairs, (none,) * LAG))
    for u in range(LAG):
        behind(PAIRS - LAG + u, carry[-1][u])


def near_kernel(list_ref, origin_ref, left_ref, mine_ref, twin_ref, total_ref, *scratch):
    total_ref[...] = jnp.zeros_like(total_ref)
    all_pairs(list_ref, origin_ref, left_ref, mine_ref, twin_ref, total_ref, scratch)


def far_kernel(
    list_ref,
    tiled_ref,
    origin_ref,
    left_ref,
    slot_ref,
    hot_ref,
    mine_ref,
    twin_ref,
    start_ref,
    out_ref,
    total_ref,
    flat_ref,
    *scratch,
):
    count = slot_ref.shape[1]
    tiles = count // LANES
    total_ref[...] = start_ref[...]
    all_pairs(list_ref, origin_ref, left_ref, mine_ref, twin_ref, total_ref, scratch)
    room = LANES // 4
    for q in range(0, tiles, 4):
        four = total_ref[q]
        for j in range(1, min(4, tiles - q)):
            four += pltpu.roll(total_ref[q + j], room * j, 1)
        flat_ref[pl.ds(q * room, LANES), :] = four.T

    def column(r):
        return flat_ref[pl.ds(r, tiles, stride=room), :]

    x, y, z = tiled_ref[0], tiled_ref[1], tiled_ref[2]
    sums = column(9) + column(10) + column(11)
    mxx, myy, mzz, mxy, mxz, myz = (column(12 + c) + column(18 + c) for c in range(6))
    const = [column(c) + column(3 + c) + column(6 + c) for c in range(3)]
    forces = [
        SCALE * (const[0] - x * sums + (mxx * x + mxy * y + mxz * z)),
        SCALE * (const[1] - y * sums + (mxy * x + myy * y + myz * z)),
        SCALE * (const[2] - z * sums + (mxz * x + myz * y + mzz * z)),
    ]
    slots = slot_ref[...]
    owner = owners(slots, tiles, count)
    parts = [part.astype(jnp.bfloat16) for force in forces for part in thirds(force)]
    got = jnp.dot(
        jnp.concatenate(parts, axis=0),
        hot_ref[...],
        preferred_element_type=jnp.float32,
    )
    for c in range(3):
        top, mid, low = (got[(3 * c + p) * tiles : (3 * c + p + 1) * tiles, :] for p in range(3))
        chosen = jnp.where(owner, top + mid + low, 0.0)
        out_ref[c : c + 1, :] = jnp.sum(chosen, axis=0, keepdims=True)


def estimate(flops):
    return pl.CostEstimate(flops=flops, bytes_accessed=10**6, transcendentals=0)


def shards(gx, gy, positions, node_moments, slot_of, block_list, tile_counts):
    count = positions.shape[1]
    tiles = count // LANES
    each = node_moments.shape[1] // LANES
    room = pl.cdiv(block_list.size + 2 * PAIRS + 1, LANES) * LANES
    vmem = pl.BlockSpec(memory_space=pltpu.VMEM)
    smem = pl.BlockSpec(memory_space=pltpu.SMEM)

    def swap(value, axis, size, bits):
        return lax.ppermute(value, axis, [(i, i ^ bits) for i in range(size)])

    def work(blocks):
        shapes = [
            pltpu.VMEM((blocks * FEATURES, LANES), jnp.float32),
            pltpu.VMEM((blocks * WEIGHTS, LANES), jnp.float32),
            pltpu.VMEM((PAIRS, LANES, 2 * LANES), jnp.float32),
            pltpu.VMEM((PAIRS, 4, LANES, LANES), jnp.bfloat16),
        ]
        rows = blocks * (FEATURES + WEIGHTS) + PAIRS * 4 * LANES + tiles * 2 * LANES
        limit = min(rows * 4 * LANES + 2**21, 60 * 1024 * 1024)
        return shapes, pltpu.CompilerParams(vmem_limit_bytes=limit)

    here = jnp.stack([lax.axis_index("gx"), lax.axis_index("gy")]).astype(jnp.int32)
    prepare = pl.pallas_call(
        functools.partial(prep_kernel, gx, gy, each),
        out_shape=(
            jax.ShapeDtypeStruct((3, tiles, LANES), jnp.float32),
            jax.ShapeDtypeStruct((3, LANES), jnp.float32),
            jax.ShapeDtypeStruct((tiles, LANES, LANES), jnp.bfloat16),
            jax.ShapeDtypeStruct((1, room), jnp.int32),
            jax.ShapeDtypeStruct((1, room), jnp.int32),
            jax.ShapeDtypeStruct((10 * each, LANES), jnp.float32),
            jax.ShapeDtypeStruct((LANES, count), jnp.bfloat16),
        ),
        in_specs=[smem] + [pl.BlockSpec(memory_space=pltpu.HBM)] * 5,
        out_specs=(vmem,) * 7,
        scratch_shapes=[
            pltpu.VMEM((tiles * FEATURES, LANES), jnp.float32),
            pltpu.VMEM(block_list.shape, jnp.int32),
            pltpu.SMEM(tile_counts.shape, jnp.int32),
            pltpu.VMEM(positions.shape, jnp.float32),
            pltpu.VMEM(slot_of.shape, jnp.int32),
            pltpu.VMEM(node_moments.shape, jnp.float32),
            pltpu.SemaphoreType.DMA((5,)),
        ],
        compiler_params=pltpu.CompilerParams(vmem_limit_bytes=8 * 2**20),
        cost_estimate=estimate(10**10),
    )
    held = [
        pltpu.with_memory_space_constraint(value, pltpu.HBM)
        for value in (block_list, tile_counts, positions, slot_of, node_moments)
    ]
    tiled, origin, left, near_list, far_list, own, hot = prepare(here, *held)
    near = [swap(node_moments, "gx", gx, b) for b in range(1, gx)]
    near = jnp.stack([own] + [value.reshape(10 * each, LANES) for value in near])
    near, origin = lax.optimization_barrier((near, origin))
    far = [swap(near, "gy", gy, b) for b in range(2, gy, 2)]
    near_twin = swap(near, "gy", gy, 1)
    near_work, near_params = work(2 * gx * each)
    near_pairs = pl.pallas_call(
        near_kernel,
        out_shape=jax.ShapeDtypeStruct((tiles + 1, LANES, LANES), jnp.float32),
        in_specs=[smem] + [vmem] * 4,
        out_specs=vmem,
        scratch_shapes=near_work,
        compiler_params=near_params,
        cost_estimate=estimate(10**10),
    )
    total = near_pairs(near_list, origin, left, near, near_twin)
    far = jnp.concatenate(far, axis=0)
    far, total = lax.optimization_barrier((far, total))
    far_twin = swap(far, "gy", gy, 1)
    far_work, far_params = work((gy - 2) * gx * each)
    return pl.pallas_call(
        far_kernel,
        out_shape=jax.ShapeDtypeStruct((3, count), jnp.float32),
        in_specs=[smem] + [vmem] * 8,
        out_specs=vmem,
        scratch_shapes=[
            pltpu.VMEM((tiles + 1, LANES, LANES), jnp.float32),
            pltpu.VMEM((pl.cdiv(tiles, 4) * LANES, LANES), jnp.float32),
        ]
        + far_work,
        compiler_params=far_params,
    )(far_list, tiled, origin, left, slot_of, hot, far, far_twin, total)


def solution(mesh):
    placed = (
        P(None, ("gx", "gy")),
        P(None, ("gx", "gy")),
        P(("gx", "gy"), None),
        P(("gx", "gy"), None),
        P(("gx", "gy")),
    )

    def body(*args):
        return shards(mesh.shape["gx"], mesh.shape["gy"], *args)

    return jax.shard_map(
        body, mesh=mesh, in_specs=placed, out_specs=P(None, ("gx", "gy")), check_vma=False
    )
```
